32 devices in a mesh: gx: 4 (over y, x), gy: 8 (over z, core).
Axes of the slice: x: 2, y: 2, z: 4, core: 2. Of those that a mesh axis runs over, the one named last changes fastest.
Arguments:
- e_field: float32 [3, 128, 256, 128], P(None, 'gx', 'gy'), may hold values from -6 to 6
- h_field: float32 [3, 128, 256, 128], P(None, 'gx', 'gy'), may hold values from -6 to 6
- psi: float32 [12, 128, 256, 128], P(None, 'gx', 'gy'), may hold values from -6 to 6
- material: int32 [128, 256, 128], P('gx', 'gy'), may hold values from 0 to 7
- eps_table: float32 [8], replicated, may hold values from 1 to 1.2
- sigma_table: float32 [8], replicated, may hold values from 0 to 0.05
Outputs:
- e_out: float32 [3, 128, 256, 128], P(None, 'gx', 'gy')
- h_out: float32 [3, 128, 256, 128], P(None, 'gx', 'gy')
- psi_out: float32 [12, 128, 256, 128], P(None, 'gx', 'gy')
The draws below stay inside these ranges and needn't reach their ends.
All inputs are finite; a program needn't handle non-finite values.
Results may differ from the reference program's by a relative error of at most 0.0003.
Values sent between devices are 32-bit elements; how exact they have to be, the bound alone decides.
A program may use at most 128 MiB of HBM per device.

```python
import math
import jax
import jax.numpy as jnp
from jax import lax

NZ = 128
PML = 16
STEPS = 16
NMAT = 8
NX = 128
NY = 256


def place_ends(array, stream_key, smallest, high):
    longest = array.shape.index(max(array.shape))
    spots = []
    for shift in (0, 1):
        where = [jax.random.randint(jax.random.fold_in(stream_key, axis), (), 0, length) for axis, length in enumerate(array.shape)]
        where[longest] = (where[longest] + shift) % array.shape[longest]
        spots.append(tuple(where))
    return array.at[spots[0]].set(smallest).at[spots[1]].set(high)


def block_scale(own_key, shape, pieces, least, top_value):
    gain = 1.0
    for dim, parts in pieces:
        heights = jax.random.uniform(jax.random.fold_in(jax.random.fold_in(own_key, 6), dim), (parts,), jnp.float32, least / len(pieces), top_value / len(pieces))
        gain = gain * jnp.repeat(jnp.exp(heights), shape[dim] // parts).reshape((-1,) + (1,) * (len(shape) - 1 - dim))
    return gain


def normal_values(stream_key, dims, spread, reach, cuts=(), kind=jnp.bfloat16):
    result = jax.random.normal(stream_key, dims, jnp.float32) * spread
    if len(cuts) > 0:
        result = block_scale(stream_key, dims, cuts, -0.22, 0.18) * result
    return jnp.clip(result, min=-reach, max=reach).astype(kind)


def setup_inputs(seed: int = 0) -> dict:
    seeds = jax.random.split(jax.random.key(seed), 7)
    e_field = normal_values(seeds[0], (3, NX, NY, NZ), 1.0, 6.0, ((1, 4), (2, 8)), jnp.float32)
    h_field = normal_values(seeds[1], (3, NX, NY, NZ), 1.0, 6.0, ((1, 4), (2, 8)), jnp.float32)
    psi = normal_values(seeds[2], (12, NX, NY, NZ), 1.0, 6.0, ((1, 4), (2, 8)), jnp.float32)
    material = place_ends(jax.random.randint(seeds[3], (NX, NY, NZ), 0, NMAT), jax.random.fold_in(seeds[3], 1), 0, NMAT - 1).astype(jnp.int32)
    eps_table = jnp.clip(jnp.exp(jax.random.uniform(seeds[4], (NMAT,), jnp.float32, math.log(1.0), math.log(1.2))), 1.0, 1.2)
    sigma_table = jnp.clip(jax.random.uniform(seeds[5], (NMAT,), jnp.float32, 0.0, 0.05), 0.0, 0.05)
    return {"e_field": e_field, "h_field": h_field, "psi": psi, "material": material, "eps_table": eps_table, "sigma_table": sigma_table}


time_step = 0.5
sigma_peak = 3.0
kappa_peak = 5.0
alpha_peak = 0.05
curl_table = (((2, 1), (1, 2)), ((0, 2), (2, 0)), ((1, 0), (0, 1)))


def profile(length, offset, extent, shift_half, thickness):
    position = (offset + lax.iota(jnp.int32, length)).astype(jnp.float32) + shift_half
    slab_width = jnp.float32(thickness)
    depth_frac = jnp.maximum(jnp.maximum((slab_width - position) / slab_width, (position - (extent - slab_width)) / slab_width), 0.0)
    depth_cube = depth_frac * depth_frac * depth_frac
    sigma_value = sigma_peak * depth_cube
    kappa_value = 1.0 + (kappa_peak - 1.0) * depth_cube
    alpha_value = alpha_peak * (1.0 - depth_frac)
    decays = jnp.exp(-(sigma_value / kappa_value + alpha_value) * time_step)
    scaling = sigma_value * (decays - 1.0) / (kappa_value * (sigma_value + kappa_value * alpha_value))
    inside_slab = depth_frac > 0.0
    return jnp.where(inside_slab, decays, 0.0), jnp.where(inside_slab, scaling, 0.0), 1.0 / kappa_value


def shaped(vector, direction):
    target_shape = [1, 1, 1]
    target_shape[direction] = vector.shape[0]
    return vector.reshape(target_shape)


def forward(field, direction, following):
    shifted = lax.slice_in_dim(field, 1, field.shape[direction], axis=direction)
    return jnp.concatenate([shifted, following], axis=direction) - field


def backward(field, direction, preceding):
    shifted = lax.slice_in_dim(field, 0, field.shape[direction] - 1, axis=direction)
    return field - jnp.concatenate([preceding, shifted], axis=direction)


def zero_layer(field, direction):
    return jnp.zeros_like(lax.slice_in_dim(field, 0, 1, axis=direction))


def update_term(difference, auxiliary, coefficient, direction):
    decays, scaling, inverse = coefficient
    renewed = decays * auxiliary + scaling * difference
    return inverse * difference + renewed, renewed


def curl(difference_of, auxiliary, first_slot, coefficients, renew):
    results = []
    renewed_list = []
    for component in range(3):
        plus_pair, minus_pair = curl_table[component]
        slot = first_slot + 2 * component
        plus_value, plus_aux = renew(difference_of(plus_pair[0], plus_pair[1]), auxiliary[slot], coefficients[plus_pair[1]], plus_pair[1])
        minus_value, minus_aux = renew(difference_of(minus_pair[0], minus_pair[1]), auxiliary[slot + 1], coefficients[minus_pair[1]], minus_pair[1])
        results.append(plus_value - minus_value)
        renewed_list.append(plus_aux)
        renewed_list.append(minus_aux)
    return results, renewed_list


def material_coefficients(material, eps_table, sigma_table):
    losses = sigma_table * time_step / (2.0 * eps_table)
    keep_table = (1.0 - losses) / (1.0 + losses)
    drive_table = (time_step / eps_table) / (1.0 + losses)
    keeping = jnp.zeros(material.shape, jnp.float32)
    driving = jnp.zeros(material.shape, jnp.float32)
    for number in range(NMAT):
        chosen = material == number
        keeping = keeping + jnp.where(chosen, keep_table[number], 0.0)
        driving = driving + jnp.where(chosen, drive_table[number], 0.0)
    return keeping, driving


def reference(e_field, h_field, psi, material, eps_table, sigma_table):
    extents = (NX, NY, NZ)
    magnetic_coef = [tuple(shaped(vector, direction) for vector in profile(extents[direction], 0, extents[direction], 0.5, PML)) for direction in range(3)]
    electric_coef = [tuple(shaped(vector, direction) for vector in profile(extents[direction], 0, extents[direction], 0.0, PML)) for direction in range(3)]
    keeping, driving = material_coefficients(material, eps_table, sigma_table)

    def advance(turn_index, carry):
        electric, magnetic, auxiliary = carry

        def electric_ahead(source, direction):
            field = electric[source]
            return forward(field, direction, zero_layer(field, direction))

        curl_h, renewed_h = curl(electric_ahead, auxiliary, 0, magnetic_coef, update_term)
        magnetic_new = jnp.stack([magnetic[component] - time_step * curl_h[component] for component in range(3)])

        def magnetic_behind(source, direction):
            field = magnetic_new[source]
            return backward(field, direction, zero_layer(field, direction))

        curl_e, renewed_e = curl(magnetic_behind, auxiliary, 6, electric_coef, update_term)
        electric_new = jnp.stack([keeping * electric[component] + driving * curl_e[component] for component in range(3)])
        return (electric_new, magnetic_new, jnp.stack(renewed_h + renewed_e))

    e_out, h_out, psi_out = lax.fori_loop(0, STEPS, advance, (e_field, h_field, psi))
    return (e_out, h_out, psi_out)
```

```python
import jax
import jax.numpy as jnp
from jax import lax
from jax.experimental import pallas as pl
from jax.experimental.pallas import tpu as pltpu
from jax.sharding import PartitionSpec as P

PML = 16
STEPS = 16
NMAT = 8
SUB = 8
GROUP = 16
AHEAD = 2

time_step = 0.5
sigma_peak = 3.0
kappa_peak = 5.0
alpha_peak = 0.05
MESH = pl.DeviceIdType.MESH


def profile(index, extent, shift_half):
    position = index.astype(jnp.float32) + shift_half
    slab_width = float(PML)
    depth_frac = jnp.maximum(
        jnp.maximum(
            (slab_width - position) / slab_width, (position - (extent - slab_width)) / slab_width
        ),
        0.0,
    )
    depth_cube = depth_frac * depth_frac * depth_frac
    sigma_value = sigma_peak * depth_cube
    kappa_value = 1.0 + (kappa_peak - 1.0) * depth_cube
    alpha_value = alpha_peak * (1.0 - depth_frac)
    decays = jnp.exp(-(sigma_value / kappa_value + alpha_value) * time_step)
    scaling = (
        sigma_value * (decays - 1.0) / (kappa_value * (sigma_value + kappa_value * alpha_value))
    )
    inside_slab = depth_frac > 0.0
    return (
        jnp.where(inside_slab, decays, 0.0),
        jnp.where(inside_slab, scaling, 0.0),
        1.0 / kappa_value,
    )


def make_kernel(size_x, size_y, rows_x, rows_y, depth_z):
    groups = rows_x // GROUP
    tiles = rows_y // SUB
    top, right = rows_x - 1, rows_y - 1

    def kernel(
        e_in, h_in, p_in, m_in, eps_ref, sig_ref, E, H, S,
        keep, drive, mat, cx, cy, cp, edge_x, edge_y,
        t_ex, t_ey, t_ax, t_ay, t_c0, t_c1,
        r_ex, r_ey, r_ax, r_ay, r_c0, r_c1,
        in_sem, send_sem, recv_sem,
    ):
        gx, gy = lax.axis_index("gx"), lax.axis_index("gy")
        has_lx, has_hx = gx > 0, gx < size_x - 1
        has_ly, has_hy = gy > 0, gy < size_y - 1
        slab_x = (gx == 0, gx == size_x - 1)
        slab_y = (gy == 0, gy == size_y - 1)
        lx, hx, ly, hy = gx - 1, gx + 1, gy - 1, gy + 1
        both = jnp.logical_and
        links = (
            (has_lx, (lx, gy)),
            (has_hx, (hx, gy)),
            (has_ly, (gx, ly)),
            (has_hy, (gx, hy)),
            (both(has_hx, has_ly), (hx, ly)),
            (both(has_lx, has_hy), (lx, hy)),
        )

        plain = [
            (e_in, E.at[:, pl.ds(0, rows_x), pl.ds(0, rows_y), :]),
            (h_in, H.at[:, pl.ds(1, rows_x), pl.ds(SUB, rows_y), :]),
            (m_in, mat),
            (p_in.at[pl.ds(1, 2)], S.at[pl.ds(1, 2)]),
            (p_in.at[pl.ds(7, 2)], S.at[pl.ds(7, 2)]),
        ]
        copies = [pltpu.make_async_copy(a, b, in_sem.at[n]) for n, (a, b) in enumerate(plain)]
        for c in copies:
            c.start()

        def slab_copies(side):
            half_x = pl.ds(side * PML, PML)
            xs = [
                pltpu.make_async_copy(
                    p_in.at[pl.ds(s, 2), half_x], S.at[pl.ds(s, 2), half_x], in_sem.at[5 + n]
                )
                for n, s in enumerate((3, 9))
            ]
            ys = [
                pltpu.make_async_copy(
                    p_in.at[s, :, half_x], S.at[s, :, half_x], in_sem.at[7 + n]
                )
                for n, s in enumerate((0, 5, 6, 11))
            ]
            return xs, ys

        for side in (0, 1):
            xs, ys = slab_copies(side)

            @pl.when(slab_x[side])
            def _():
                for c in xs:
                    c.start()

            @pl.when(slab_y[side])
            def _():
                for c in ys:
                    c.start()

        for ref in (r_ex, r_ey, r_ax, r_ay, r_c0, r_c1):
            ref[...] = jnp.zeros(ref.shape, jnp.float32)

        barrier = pltpu.get_barrier_semaphore()
        for present, target in links:

            @pl.when(present)
            def _():
                pl.semaphore_signal(barrier, inc=1, device_id=target, device_id_type=MESH)

        zero = jnp.zeros((SUB, depth_z), jnp.float32)
        for side in (0, 1):

            @pl.when(jnp.logical_not(slab_x[side]))
            def _():
                @pl.loop(side * PML, side * PML + PML)
                def _(i):
                    for s in (3, 4, 9, 10):
                        S[s, i] = jnp.zeros((rows_y, depth_z), jnp.float32)

            @pl.when(jnp.logical_not(slab_y[side]))
            def _():
                @pl.loop(0, rows_x)
                def _(i):
                    for s in (0, 5, 6, 11):
                        S[s, i, pl.ds(side * PML, PML), :] = jnp.zeros(
                            (PML, depth_z), jnp.float32
                        )

        for c in range(3):
            for t in range(tiles):
                E[c, rows_x, pl.ds(t * SUB, SUB), :] = zero
                H[c, 0, pl.ds(SUB + t * SUB, SUB), :] = zero

        @pl.loop(0, rows_x)
        def _(i):
            for c in range(3):
                E[c, i, pl.ds(rows_y, SUB), :] = zero
                H[c, i + 1, pl.ds(0, SUB), :] = zero

        lane = lax.broadcasted_iota(jnp.int32, (SUB, depth_z), 1)
        row = lax.broadcasted_iota(jnp.int32, (rows_y, depth_z), 0)
        column = lax.broadcasted_iota(jnp.int32, (rows_x, depth_z), 0)
        plane = lax.broadcasted_iota(jnp.int32, (rows_x, SUB, depth_z), 0)
        zc = []
        for k, shift in enumerate((0.5, 0.0)):
            zc.append(profile(lane, depth_z, shift))
            for n, v in enumerate(profile(row + gy * rows_y, size_y * rows_y, shift)):
                cy[k, n] = v
            for n, v in enumerate(profile(plane + gx * rows_x, size_x * rows_x, shift)):
                cx[k, n] = v
            for n, v in enumerate(profile(column + gx * rows_x, size_x * rows_x, shift)):
                cp[k, n] = v
        not_last = lane < depth_z - 1
        not_first = lane > 0

        keep_vals, drive_vals = [], []
        for m in range(NMAT):
            eps = jnp.full((SUB, depth_z), eps_ref[m], jnp.float32)
            sig = jnp.full((SUB, depth_z), sig_ref[m], jnp.float32)
            loss = sig * time_step / (2.0 * eps)
            keep_vals.append((1.0 - loss) / (1.0 + loss))
            drive_vals.append((time_step / eps) / (1.0 + loss))
        copies[2].wait()

        @pl.loop(0, rows_x)
        def _(i):
            for t in range(tiles):
                rows = pl.ds(t * SUB, SUB)
                number = mat[i, rows, :]
                kv, dv = keep_vals[0], drive_vals[0]
                for m in range(1, NMAT):
                    chosen = number == m
                    kv = jnp.where(chosen, keep_vals[m], kv)
                    dv = jnp.where(chosen, drive_vals[m], dv)
                keep[i, rows, :] = kv
                drive[i, rows, :] = dv

        for n in (0, 1, 3, 4):
            copies[n].wait()
        for side in (0, 1):
            xs, ys = slab_copies(side)

            @pl.when(slab_x[side])
            def _():
                for c in xs:
                    c.wait()

            @pl.when(slab_y[side])
            def _():
                for c in ys:
                    c.wait()

        pl.semaphore_wait(barrier, sum(jnp.where(present, 1, 0) for present, _t in links))

        def term(old, d, coef):
            b, a, q = coef
            renewed = b * old + a * d
            return q * d + renewed, renewed

        def loads(k, i, y, in_x, in_y):
            rows, at = pl.ds(y, SUB), pl.ds(y + SUB, SUB)
            first = 6 * k
            if k == 0:
                src, j, now, step, line = E, i, rows, 1, pl.ds(y + 1, SUB)
                old = [H[c, i + 1, at, :] for c in range(3)]
                mats = ()
            else:
                src, j, now, step, line = H, i + 1, at, -1, pl.ds(y + SUB - 1, SUB)
                old = [E[c, i, rows, :] for c in range(3)]
                mats = (keep[i, rows, :], drive[i, rows, :])
            own = [src[c, j, now, :] for c in range(3)]
            side_x = [src[c, j + step, now, :] for c in (1, 2)]
            side_y = [src[c, j, line, :] for c in (0, 2)]
            slots = [1, 2] + ([3, 4] if in_x else []) + ([0, 5] if in_y else [])
            aux = {n: S[first + n, i, rows, :] for n in slots}
            coef_x = [cx[k, n, i] for n in range(3)] if in_x else None
            return own, side_x, side_y, old, mats, aux, coef_x

        def compute(k, values, coef_y):
            own, (x1, x2), (y0, y2), old, mats, aux, coef_x = values
            f0, f1, f2 = own
            if k == 0:
                dx1, dx2, dy0, dy2 = x1 - f1, x2 - f2, y0 - f0, y2 - f2
                dz0 = jnp.where(not_last, pltpu.roll(f0, depth_z - 1, 1), 0.0) - f0
                dz1 = jnp.where(not_last, pltpu.roll(f1, depth_z - 1, 1), 0.0) - f1
            else:
                dx1, dx2, dy0, dy2 = f1 - x1, f2 - x2, f0 - y0, f2 - y2
                dz0 = f0 - jnp.where(not_first, pltpu.roll(f0, 1, 1), 0.0)
                dz1 = f1 - jnp.where(not_first, pltpu.roll(f1, 1, 1), 0.0)
            fresh = {}
            dz1, fresh[1] = term(aux[1], dz1, zc[k])
            dz0, fresh[2] = term(aux[2], dz0, zc[k])
            if coef_x is not None:
                dx2, fresh[3] = term(aux[3], dx2, coef_x)
                dx1, fresh[4] = term(aux[4], dx1, coef_x)
            if coef_y is not None:
                dy2, fresh[0] = term(aux[0], dy2, coef_y)
                dy0, fresh[5] = term(aux[5], dy0, coef_y)
            curls = (dy2 - dz1, dz0 - dx2, dx1 - dy0)
            if k == 0:
                return [o - time_step * c for o, c in zip(old, curls)], fresh
            return [mats[0] * o + mats[1] * c for o, c in zip(old, curls)], fresh

        def stores(k, i, y, result):
            fields, fresh = result
            for c in range(3):
                if k == 0:
                    H[c, i + 1, pl.ds(y + SUB, SUB), :] = fields[c]
                else:
                    E[c, i, pl.ds(y, SUB), :] = fields[c]
            for n, v in fresh.items():
                S[6 * k + n, i, pl.ds(y, SUB), :] = v

        def run(k, i0, y, in_x, in_y):
            coef_y = [cy[k, n, pl.ds(y, SUB), :] for n in range(3)] if in_y else None
            ready = [loads(k, i0 + u, y, in_x, in_y) for u in range(AHEAD)]
            for u in range(GROUP):
                if u + AHEAD < GROUP:
                    ready.append(loads(k, i0 + u + AHEAD, y, in_x, in_y))
                stores(k, i0 + u, y, compute(k, ready[u], coef_y))

        def unit(k, g, t):
            low_x, low_y = g * GROUP < PML, t * SUB < PML
            px = jnp.where(low_x, slab_x[0], slab_x[1])
            py = jnp.where(low_y, slab_y[0], slab_y[1])
            i0, y = g * GROUP, pl.multiple_of(t * SUB, SUB)

            def split_y(in_x):
                lax.cond(
                    py,
                    lambda: run(k, i0, y, in_x, True),
                    lambda: run(k, i0, y, in_x, False),
                )

            lax.cond(px, lambda: split_y(True), lambda: split_y(False))

        def exchange(s):
            moves = (
                (has_lx, (lx, gy), has_hx, t_ex, r_ex),
                (has_hx, (hx, gy), has_lx, t_ax, r_ax),
                (both(has_hx, has_ly), (hx, ly), both(has_lx, has_hy), t_c0, r_c0),
                (both(has_lx, has_hy), (lx, hy), both(has_hx, has_ly), t_c1, r_c1),
                (has_ly, (gx, ly), has_hy, t_ey, r_ey),
                (has_hy, (gx, hy), has_ly, t_ay, r_ay),
            )
            made = [
                (
                    sends,
                    gets,
                    pltpu.make_async_remote_copy(
                        src_ref=src,
                        dst_ref=dst.at[s],
                        send_sem=send_sem.at[n],
                        recv_sem=recv_sem.at[n, s],
                        device_id=target,
                        device_id_type=MESH,
                    ),
                )
                for n, (sends, target, gets, src, dst) in enumerate(moves)
            ]
            return made[:4], made[4:]

        own = pl.ds(0, rows_y)
        inner = pl.ds(SUB, rows_y)
        half = time_step
        wide = rows_y + SUB
        flat_e = E.reshape(3 * (rows_x + 1) * wide, depth_z)
        flat_h = H.reshape(3 * (rows_x + 1) * wide, depth_z)
        flat_s = S.reshape(12 * rows_x * rows_y, depth_z)
        flat_keep = keep.reshape(rows_x * rows_y, depth_z)
        flat_drive = drive.reshape(rows_x * rows_y, depth_z)
        packs = rows_x // SUB

        def across(c, i, y):
            return pl.ds((c * (rows_x + 1) + i) * wide + y, SUB, stride=wide)

        def within(c, i, y):
            return pl.ds((c * rows_x + i) * rows_y + y, SUB, stride=rows_y)

        def start(moves):
            for sends, _g, copy in moves:

                @pl.when(sends)
                def _():
                    copy.start()

        def finish(moves):
            for sends, gets, copy in moves:

                @pl.when(gets)
                def _():
                    copy.wait_recv()

                @pl.when(sends)
                def _():
                    copy.wait_send()

        def coefs_y(k, y):
            return [cy[k, n, pl.ds(y, SUB), :] for n in range(3)]

        def faces_x():
            late = []
            for t in range(tiles):
                y = t * SUB
                fields, _f = compute(1, loads(1, 0, y, False, True), coefs_y(1, y))
                t_ex[0, pl.ds(y, SUB), :] = fields[1]
                t_ex[1, pl.ds(y, SUB), :] = fields[2]
                if t == tiles - 1:
                    t_c1[...] = fields[1]
                fields, _f = compute(1, loads(1, top, y, False, True), coefs_y(1, y))
                edge_x[pl.ds(y, SUB), :] = fields[0]
                if t == 0:
                    t_c0[...] = fields[0]
                late.append(fields)
            for t in range(tiles):
                y = t * SUB
                rows, at = pl.ds(y, SUB), pl.ds(y + SUB, SUB)
                old = [H[c, rows_x, at, :] for c in range(3)]
                aux = {n: S[n, top, rows, :] for n in (1, 2, 0, 5)}
                side_y = (edge_x[pl.ds(y + 1, SUB), :], zero)
                values = (late[t], (zero, zero), side_y, old, (), aux, None)
                fields, _f = compute(0, values, coefs_y(0, y))
                t_ax[0, rows, :] = fields[1]
                t_ax[1, rows, :] = fields[2]

        def packed_e(r, u):
            i = u * SUB
            own_h = [flat_h[across(c, i + 1, SUB + r), :] for c in range(3)]
            side_x = [flat_h[across(c, i, SUB + r), :] for c in (1, 2)]
            side_y = [flat_h[across(c, i + 1, SUB + r - 1), :] for c in (0, 2)]
            old = [flat_e[across(c, i, r), :] for c in range(3)]
            mats = (flat_keep[within(0, i, r), :], flat_drive[within(0, i, r), :])
            aux = {n: flat_s[within(6 + n, i, r), :] for n in (1, 2, 3, 4)}
            coef_x = [cp[1, n, pl.ds(i, SUB), :] for n in range(3)]
            return compute(1, (own_h, side_x, side_y, old, mats, aux, coef_x), None)[0]

        def faces_y():
            late = []
            for u in range(packs):
                rows = pl.ds(u * SUB, SUB)
                fields = packed_e(0, u)
                t_ey[0, rows, :] = fields[0]
                t_ey[1, rows, :] = fields[2]
                fields = packed_e(right, u)
                edge_y[rows, :] = fields[1]
                late.append(fields)
            for u in range(packs):
                i = u * SUB
                rows = pl.ds(i, SUB)
                old = [flat_h[across(c, i + 1, SUB + right), :] for c in range(3)]
                aux = {n: flat_s[within(n, i, right), :] for n in (1, 2, 3, 4)}
                coef_x = [cp[0, n, rows, :] for n in range(3)]
                side_x = (edge_y[pl.ds(i + 1, SUB), :], zero)
                values = (late[u], side_x, (zero, zero), old, (), aux, coef_x)
                fields, _f = compute(0, values, None)
                t_ay[0, rows, :] = fields[0]
                t_ay[1, rows, :] = fields[2]

        def sweep(k, count):
            @pl.loop(0, count)
            def _(n):
                unit(k, lax.div(n, tiles), lax.rem(n, tiles))

        def fix_y(s):
            @pl.when(has_hy)
            def _():
                for u in range(packs):
                    i = u * SUB
                    rows = pl.ds(i, SUB)
                    a0, a2 = across(0, i + 1, SUB + right), across(2, i + 1, SUB + right)
                    flat_h[a0, :] = flat_h[a0, :] - half * r_ey[s, 1, rows, :]
                    flat_h[a2, :] = flat_h[a2, :] + half * r_ey[s, 0, rows, :]

            @pl.when(has_ly)
            def _():
                for u in range(packs):
                    i = u * SUB
                    rows = pl.ds(i, SUB)
                    e0, e2 = flat_e[across(0, i, 0), :], flat_e[across(2, i, 0), :]
                    flat_h[across(0, i + 1, SUB - 1), :] = r_ay[s, 0, rows, :] - half * e2
                    flat_h[across(2, i + 1, SUB - 1), :] = r_ay[s, 1, rows, :] + half * e0

        def fix_x(s):
            @pl.when(has_ly)
            def _():
                edge = pl.ds(SUB - 1, 1)
                H[2, rows_x, edge, :] = (
                    H[2, rows_x, edge, :] - half * r_c1[s, pl.ds(SUB - 1, 1), :]
                )

            @pl.when(has_hx)
            def _():
                H[1, rows_x, inner, :] = H[1, rows_x, inner, :] + half * r_ex[s, 1]
                H[2, rows_x, inner, :] = H[2, rows_x, inner, :] - half * r_ex[s, 0]

            @pl.when(has_lx)
            def _():
                H[1, 0, inner, :] = r_ax[s, 0] + half * E[2, 0, own, :]
                H[2, 0, inner, :] = r_ax[s, 1] - half * E[1, 0, own, :]
                edge = pl.ds(SUB + right, 1)
                H[2, 0, edge, :] = H[2, 0, edge, :] + half * r_c0[s, pl.ds(0, 1), :]

        edge_x[pl.ds(rows_y, SUB), :] = zero
        edge_y[pl.ds(rows_x, SUB), :] = zero
        count = groups * tiles
        sweep(0, count)
        t_ex[0] = E[1, 0, own, :]
        t_ex[1] = E[2, 0, own, :]
        t_ax[0] = H[1, rows_x, inner, :]
        t_ax[1] = H[2, rows_x, inner, :]
        t_c0[...] = E[0, top, pl.ds(0, SUB), :]
        t_c1[...] = E[1, 0, pl.ds(rows_y - SUB, SUB), :]
        for u in range(packs):
            i = u * SUB
            rows = pl.ds(i, SUB)
            t_ey[0, rows, :] = flat_e[across(0, i, 0), :]
            t_ey[1, rows, :] = flat_e[across(2, i, 0), :]
            t_ay[0, rows, :] = flat_h[across(0, i + 1, SUB + right), :]
            t_ay[1, rows, :] = flat_h[across(2, i + 1, SUB + right), :]
        first_x, first_y = exchange(0)
        start(first_x)
        start(first_y)

        def advance(step, carry):
            s = lax.rem(step, 2)
            old_x, old_y = exchange(s)
            new_x, new_y = exchange(1 - s)
            more = step < STEPS - 1
            finish(old_y)
            fix_y(s)
            finish(old_x)
            fix_x(s)

            @pl.when(more)
            def _():
                faces_x()
                start(new_x)
                faces_y()
                start(new_y)

            sweep(1, count)
            sweep(0, jnp.where(more, count, 0))
            return carry

        lax.fori_loop(0, STEPS, advance, 0)

    return kernel


def make_writer(rows_x, rows_y):
    def writer(E, H, S, e_out, h_out, p_out, out_sem):
        outs = [
            pltpu.make_async_copy(
                E.at[:, pl.ds(0, rows_x), pl.ds(0, rows_y), :], e_out, out_sem.at[0]
            ),
            pltpu.make_async_copy(
                H.at[:, pl.ds(1, rows_x), pl.ds(SUB, rows_y), :], h_out, out_sem.at[1]
            ),
            pltpu.make_async_copy(S, p_out, out_sem.at[2]),
        ]
        for c in outs:
            c.start()
        for c in outs:
            c.wait()

    return writer


def solution(mesh):
    size_x, size_y = mesh.shape["gx"], mesh.shape["gy"]

    def shards(e_field, h_field, psi, material, eps_table, sigma_table):
        _, rows_x, rows_y, depth_z = e_field.shape
        assert rows_x == 2 * PML and rows_y == 2 * PML and size_x > 1 and size_y > 1
        f32 = jnp.float32
        any_space = pl.BlockSpec(memory_space=pltpu.HBM)
        smem = pl.BlockSpec(memory_space=pltpu.SMEM)
        face_x = (2, rows_y, depth_z)
        face_y = (2, rows_x, depth_z)
        corner = (SUB, depth_z)
        faces = (face_x, face_y, face_x, face_y, corner, corner)
        padded = (3, rows_x + 1, rows_y + SUB, depth_z)
        cell = (rows_x, rows_y, depth_z)
        vmem = pl.BlockSpec(memory_space=pltpu.VMEM)
        state = pl.pallas_call(
            make_kernel(size_x, size_y, rows_x, rows_y, depth_z),
            out_shape=[pltpu.VMEM(padded, f32), pltpu.VMEM(padded, f32), pltpu.VMEM(psi.shape, f32)],
            in_specs=[any_space] * 4 + [smem] * 2,
            out_specs=[vmem] * 3,
            scratch_shapes=[
                pltpu.VMEM(cell, f32),
                pltpu.VMEM(cell, f32),
                pltpu.VMEM(cell, jnp.int32),
                pltpu.VMEM((2, 3, rows_x, SUB, depth_z), f32),
                pltpu.VMEM((2, 3, rows_y, depth_z), f32),
                pltpu.VMEM((2, 3, rows_x, depth_z), f32),
                pltpu.VMEM((rows_y + SUB, depth_z), f32),
                pltpu.VMEM((rows_x + SUB, depth_z), f32),
            ]
            + [pltpu.VMEM(f, f32) for f in faces]
            + [pltpu.VMEM((2,) + f, f32) for f in faces]
            + [
                pltpu.SemaphoreType.DMA((11,)),
                pltpu.SemaphoreType.DMA((6,)),
                pltpu.SemaphoreType.DMA((6, 2)),
            ],
            compiler_params=pltpu.CompilerParams(
                collective_id=0, has_side_effects=True, vmem_limit_bytes=53 << 20
            ),
        )(e_field, h_field, psi, material, eps_table, sigma_table)
        return pl.pallas_call(
            make_writer(rows_x, rows_y),
            out_shape=[jax.ShapeDtypeStruct(a.shape, f32) for a in (e_field, h_field, psi)],
            in_specs=[vmem] * 3,
            out_specs=[any_space] * 3,
            scratch_shapes=[pltpu.SemaphoreType.DMA((3,))],
            compiler_params=pltpu.CompilerParams(vmem_limit_bytes=24 << 20),
        )(*state)

    split = P(None, "gx", "gy", None)
    return jax.shard_map(
        shards,
        mesh=mesh,
        in_specs=(split, split, split, P("gx", "gy", None), P(), P()),
        out_specs=(split, split, split),
        check_vma=False,
    )
```

```python
import jax
import jax.numpy as jnp
from jax import lax
from jax.experimental import pallas as pl
from jax.experimental.pallas import tpu as pltpu
from jax.sharding import PartitionSpec as P

PML = 16
STEPS = 16
NMAT = 8
SUB = 8
GROUP = 16
AHEAD = 2

time_step = 0.5
sigma_peak = 3.0
kappa_peak = 5.0
alpha_peak = 0.05
MESH = pl.DeviceIdType.MESH


def profile(index, extent, shift_half):
    position = index.astype(jnp.float32) + shift_half
    slab_width = float(PML)
    depth_frac = jnp.maximum(
        jnp.maximum(
            (slab_width - position) / slab_width, (position - (extent - slab_width)) / slab_width
        ),
        0.0,
    )
    depth_cube = depth_frac * depth_frac * depth_frac
    sigma_value = sigma_peak * depth_cube
    kappa_value = 1.0 + (kappa_peak - 1.0) * depth_cube
    alpha_value = alpha_peak * (1.0 - depth_frac)
    decays = jnp.exp(-(sigma_value / kappa_value + alpha_value) * time_step)
    scaling = (
        sigma_value * (decays - 1.0) / (kappa_value * (sigma_value + kappa_value * alpha_value))
    )
    inside_slab = depth_frac > 0.0
    return (
        jnp.where(inside_slab, decays, 0.0),
        jnp.where(inside_slab, scaling, 0.0),
        1.0 / kappa_value,
    )


def make_kernel(size_x, size_y, rows_x, rows_y, depth_z):
    groups = rows_x // GROUP
    tiles = rows_y // SUB
    top, right = rows_x - 1, rows_y - 1

    def kernel(
        e_in, h_in, p_in, m_in, eps_ref, sig_ref, E, H, S,
        keep, drive, mat, cx, cy, cp, edge_x, edge_y,
        t_ex, t_ey, t_ax, t_ay, t_c0, t_c1,
        r_ex, r_ey, r_ax, r_ay, r_c0, r_c1,
        in_sem, send_sem, recv_sem,
    ):
        gx, gy = lax.axis_index("gx"), lax.axis_index("gy")
        has_lx, has_hx = gx > 0, gx < size_x - 1
        has_ly, has_hy = gy > 0, gy < size_y - 1
        slab_x = (gx == 0, gx == size_x - 1)
        slab_y = (gy == 0, gy == size_y - 1)
        lx, hx, ly, hy = gx - 1, gx + 1, gy - 1, gy + 1
        both = jnp.logical_and
        links = (
            (has_lx, (lx, gy)),
            (has_hx, (hx, gy)),
            (has_ly, (gx, ly)),
            (has_hy, (gx, hy)),
            (both(has_hx, has_ly), (hx, ly)),
            (both(has_lx, has_hy), (lx, hy)),
        )

        def field_copies():
            pairs = (
                (e_in, E.at[:, pl.ds(0, rows_x), pl.ds(0, rows_y), :]),
                (h_in, H.at[:, pl.ds(1, rows_x), pl.ds(SUB, rows_y), :]),
                (m_in, mat),
            )
            return [pltpu.make_async_copy(a, b, in_sem.at[n]) for n, (a, b) in enumerate(pairs)]

        def slot_copies(k):
            first, base = 6 * k, 3 + 7 * k
            pair = pl.ds(first + 1, 2)
            always = pltpu.make_async_copy(p_in.at[pair], S.at[pair], in_sem.at[base])
            guarded = []
            for side in (0, 1):
                half_x, pair = pl.ds(side * PML, PML), pl.ds(first + 3, 2)
                guarded.append(
                    (
                        slab_x[side],
                        pltpu.make_async_copy(
                            p_in.at[pair, half_x], S.at[pair, half_x], in_sem.at[base + 1 + side]
                        ),
                    )
                )
                for n, slot in enumerate((first, first + 5)):
                    guarded.append(
                        (
                            slab_y[side],
                            pltpu.make_async_copy(
                                p_in.at[slot, :, half_x],
                                S.at[slot, :, half_x],
                                in_sem.at[base + 3 + 2 * side + n],
                            ),
                        )
                    )
            return always, guarded

        def start_slots(k):
            always, guarded = slot_copies(k)
            always.start()
            for present, copy in guarded:

                @pl.when(present)
                def _():
                    copy.start()

        def wait_slots(k):
            always, guarded = slot_copies(k)
            always.wait()
            for present, copy in guarded:

                @pl.when(present)
                def _():
                    copy.wait()

        fields_in = field_copies()
        fields_in[0].start()
        fields_in[1].start()
        start_slots(0)
        fields_in[2].start()
        start_slots(1)

        barrier = pltpu.get_barrier_semaphore()
        for present, target in links:

            @pl.when(present)
            def _():
                pl.semaphore_signal(barrier, inc=1, device_id=target, device_id_type=MESH)

        zero = jnp.zeros((SUB, depth_z), jnp.float32)
        for side in (0, 1):

            @pl.when(jnp.logical_not(slab_x[side]))
            def _():
                @pl.loop(side * PML, side * PML + PML)
                def _(i):
                    for s in (3, 4, 9, 10):
                        S[s, i] = jnp.zeros((rows_y, depth_z), jnp.float32)

            @pl.when(jnp.logical_not(slab_y[side]))
            def _():
                @pl.loop(0, rows_x)
                def _(i):
                    for s in (0, 5, 6, 11):
                        S[s, i, pl.ds(side * PML, PML), :] = jnp.zeros(
                            (PML, depth_z), jnp.float32
                        )

        for c in range(3):
            for t in range(tiles):
                E[c, rows_x, pl.ds(t * SUB, SUB), :] = zero
                H[c, 0, pl.ds(SUB + t * SUB, SUB), :] = zero

        @pl.loop(0, rows_x)
        def _(i):
            for c in range(3):
                E[c, i, pl.ds(rows_y, SUB), :] = zero
                H[c, i + 1, pl.ds(0, SUB), :] = zero

        lane = lax.broadcasted_iota(jnp.int32, (SUB, depth_z), 1)
        row = lax.broadcasted_iota(jnp.int32, (rows_y, depth_z), 0)
        column = lax.broadcasted_iota(jnp.int32, (rows_x, depth_z), 0)
        plane = lax.broadcasted_iota(jnp.int32, (rows_x, SUB, depth_z), 0)
        zc = []
        for k, shift in enumerate((0.5, 0.0)):
            zc.append(profile(lane, depth_z, shift))
            for n, v in enumerate(profile(row + gy * rows_y, size_y * rows_y, shift)):
                cy[k, n] = v
            for n, v in enumerate(profile(plane + gx * rows_x, size_x * rows_x, shift)):
                cx[k, n] = v
            for n, v in enumerate(profile(column + gx * rows_x, size_x * rows_x, shift)):
                cp[k, n] = v
        not_last = lane < depth_z - 1
        not_first = lane > 0

        def materials():
            keep_vals, drive_vals = [], []
            for m in range(NMAT):
                eps = jnp.full((SUB, depth_z), eps_ref[m], jnp.float32)
                sig = jnp.full((SUB, depth_z), sig_ref[m], jnp.float32)
                loss = sig * time_step / (2.0 * eps)
                keep_vals.append((1.0 - loss) / (1.0 + loss))
                drive_vals.append((time_step / eps) / (1.0 + loss))

            @pl.loop(0, rows_x)
            def _(i):
                for t in range(tiles):
                    rows = pl.ds(t * SUB, SUB)
                    number = mat[i, rows, :]
                    kv, dv = keep_vals[0], drive_vals[0]
                    for m in range(1, NMAT):
                        chosen = number == m
                        kv = jnp.where(chosen, keep_vals[m], kv)
                        dv = jnp.where(chosen, drive_vals[m], dv)
                    keep[i, rows, :] = kv
                    drive[i, rows, :] = dv

        def term(old, d, coef):
            b, a, q = coef
            renewed = b * old + a * d
            return q * d + renewed, renewed

        def loads(k, i, y, in_x, in_y):
            rows, at = pl.ds(y, SUB), pl.ds(y + SUB, SUB)
            first = 6 * k
            if k == 0:
                src, j, now, step, line = E, i, rows, 1, pl.ds(y + 1, SUB)
                old = [H[c, i + 1, at, :] for c in range(3)]
                mats = ()
            else:
                src, j, now, step, line = H, i + 1, at, -1, pl.ds(y + SUB - 1, SUB)
                old = [E[c, i, rows, :] for c in range(3)]
                mats = (keep[i, rows, :], drive[i, rows, :])
            own = [src[c, j, now, :] for c in range(3)]
            side_x = [src[c, j + step, now, :] for c in (1, 2)]
            side_y = [src[c, j, line, :] for c in (0, 2)]
            slots = [1, 2] + ([3, 4] if in_x else []) + ([0, 5] if in_y else [])
            aux = {n: S[first + n, i, rows, :] for n in slots}
            coef_x = [cx[k, n, i] for n in range(3)] if in_x else None
            return own, side_x, side_y, old, mats, aux, coef_x

        def compute(k, values, coef_y):
            own, (x1, x2), (y0, y2), old, mats, aux, coef_x = values
            f0, f1, f2 = own
            if k == 0:
                dx1, dx2, dy0, dy2 = x1 - f1, x2 - f2, y0 - f0, y2 - f2
                dz0 = jnp.where(not_last, pltpu.roll(f0, depth_z - 1, 1), 0.0) - f0
                dz1 = jnp.where(not_last, pltpu.roll(f1, depth_z - 1, 1), 0.0) - f1
            else:
                dx1, dx2, dy0, dy2 = f1 - x1, f2 - x2, f0 - y0, f2 - y2
                dz0 = f0 - jnp.where(not_first, pltpu.roll(f0, 1, 1), 0.0)
                dz1 = f1 - jnp.where(not_first, pltpu.roll(f1, 1, 1), 0.0)
            fresh = {}
            dz1, fresh[1] = term(aux[1], dz1, zc[k])
            dz0, fresh[2] = term(aux[2], dz0, zc[k])
            if coef_x is not None:
                dx2, fresh[3] = term(aux[3], dx2, coef_x)
                dx1, fresh[4] = term(aux[4], dx1, coef_x)
            if coef_y is not None:
                dy2, fresh[0] = term(aux[0], dy2, coef_y)
                dy0, fresh[5] = term(aux[5], dy0, coef_y)
            curls = (dy2 - dz1, dz0 - dx2, dx1 - dy0)
            if k == 0:
                return [o - time_step * c for o, c in zip(old, curls)], fresh
            return [mats[0] * o + mats[1] * c for o, c in zip(old, curls)], fresh

        def stores(k, i, y, result):
            fields, fresh = result
            for c in range(3):
                if k == 0:
                    H[c, i + 1, pl.ds(y + SUB, SUB), :] = fields[c]
                else:
                    E[c, i, pl.ds(y, SUB), :] = fields[c]
            for n, v in fresh.items():
                S[6 * k + n, i, pl.ds(y, SUB), :] = v

        def run(k, i0, y, in_x, in_y):
            coef_y = [cy[k, n, pl.ds(y, SUB), :] for n in range(3)] if in_y else None
            ready = [loads(k, i0 + u, y, in_x, in_y) for u in range(AHEAD)]
            for u in range(GROUP):
                if u + AHEAD < GROUP:
                    ready.append(loads(k, i0 + u + AHEAD, y, in_x, in_y))
                stores(k, i0 + u, y, compute(k, ready[u], coef_y))

        def unit(k, g, t):
            low_x, low_y = g * GROUP < PML, t * SUB < PML
            px = jnp.where(low_x, slab_x[0], slab_x[1])
            py = jnp.where(low_y, slab_y[0], slab_y[1])
            i0, y = g * GROUP, pl.multiple_of(t * SUB, SUB)

            def split_y(in_x):
                lax.cond(
                    py,
                    lambda: run(k, i0, y, in_x, True),
                    lambda: run(k, i0, y, in_x, False),
                )

            lax.cond(px, lambda: split_y(True), lambda: split_y(False))

        def exchange(s):
            one, last = pl.ds(0, 1), pl.ds(SUB - 1, 1)
            diag_c0, diag_c1 = both(has_hx, has_ly), both(has_lx, has_hy)
            moves = (
                (diag_c0, (hx, ly), diag_c1, t_c0.at[one], r_c0.at[s, one]),
                (has_hx, (hx, gy), has_lx, t_ax, r_ax.at[s]),
                (diag_c1, (lx, hy), diag_c0, t_c1.at[last], r_c1.at[s, last]),
                (has_lx, (lx, gy), has_hx, t_ex, r_ex.at[s]),
                (has_ly, (gx, ly), has_hy, t_ey, r_ey.at[s]),
                (has_hy, (gx, hy), has_ly, t_ay, r_ay.at[s]),
            )
            made = [
                (
                    sends,
                    gets,
                    pltpu.make_async_remote_copy(
                        src_ref=src,
                        dst_ref=dst,
                        send_sem=send_sem.at[n],
                        recv_sem=recv_sem.at[n, s],
                        device_id=target,
                        device_id_type=MESH,
                    ),
                )
                for n, (sends, target, gets, src, dst) in enumerate(moves)
            ]
            return made[:2], made[2:4], made[4:]

        own = pl.ds(0, rows_y)
        inner = pl.ds(SUB, rows_y)
        half = time_step
        wide = rows_y + SUB
        flat_e = E.reshape(3 * (rows_x + 1) * wide, depth_z)
        flat_h = H.reshape(3 * (rows_x + 1) * wide, depth_z)
        flat_s = S.reshape(12 * rows_x * rows_y, depth_z)
        flat_keep = keep.reshape(rows_x * rows_y, depth_z)
        flat_drive = drive.reshape(rows_x * rows_y, depth_z)
        packs = rows_x // SUB

        def across(c, i, y):
            return pl.ds((c * (rows_x + 1) + i) * wide + y, SUB, stride=wide)

        def within(c, i, y):
            return pl.ds((c * rows_x + i) * rows_y + y, SUB, stride=rows_y)

        def start(moves):
            for sends, _g, copy in moves:

                @pl.when(sends)
                def _():
                    copy.start()

        def arrived(moves):
            for _s, gets, copy in moves:

                @pl.when(gets)
                def _():
                    copy.wait_recv()

        def left(moves):
            for sends, _g, copy in moves:

                @pl.when(sends)
                def _():
                    copy.wait_send()

        def coefs_y(k, y):
            return [cy[k, n, pl.ds(y, SUB), :] for n in range(3)]

        def face_low():
            for t in range(tiles):
                y = t * SUB
                fields, _f = compute(1, loads(1, 0, y, False, True), coefs_y(1, y))
                t_ex[0, pl.ds(y, SUB), :] = fields[1]
                t_ex[1, pl.ds(y, SUB), :] = fields[2]
                if t == tiles - 1:
                    t_c1[...] = fields[1]

        def face_high():
            fields = []
            for t in range(tiles):
                y = t * SUB
                fields.append(compute(1, loads(1, top, y, False, True), coefs_y(1, y))[0])
            partial_high(fields)

        def partial_high(e_new):
            t_c0[...] = e_new[0][0]
            for t in range(tiles):
                edge_x[pl.ds(t * SUB, SUB), :] = e_new[t][0]
            for t in range(tiles):
                y = t * SUB
                rows, at = pl.ds(y, SUB), pl.ds(y + SUB, SUB)
                old = [H[c, rows_x, at, :] for c in range(3)]
                aux = {n: S[n, top, rows, :] for n in (1, 2, 0, 5)}
                side_y = (edge_x[pl.ds(y + 1, SUB), :], zero)
                values = (e_new[t], (zero, zero), side_y, old, (), aux, None)
                fields, _f = compute(0, values, coefs_y(0, y))
                t_ax[0, rows, :] = fields[1]
                t_ax[1, rows, :] = fields[2]

        def packed_e(r, u):
            i = u * SUB
            own_h = [flat_h[across(c, i + 1, SUB + r), :] for c in range(3)]
            side_x = [flat_h[across(c, i, SUB + r), :] for c in (1, 2)]
            side_y = [flat_h[across(c, i + 1, SUB + r - 1), :] for c in (0, 2)]
            old = [flat_e[across(c, i, r), :] for c in range(3)]
            mats = (flat_keep[within(0, i, r), :], flat_drive[within(0, i, r), :])
            aux = {n: flat_s[within(6 + n, i, r), :] for n in (1, 2, 3, 4)}
            coef_x = [cp[1, n, pl.ds(i, SUB), :] for n in range(3)]
            return compute(1, (own_h, side_x, side_y, old, mats, aux, coef_x), None)[0]

        def faces_y():
            late = []
            for u in range(packs):
                rows = pl.ds(u * SUB, SUB)
                fields = packed_e(0, u)
                t_ey[0, rows, :] = fields[0]
                t_ey[1, rows, :] = fields[2]
                late.append(packed_e(right, u))
            partial_y(late)

        def partial_y(e_new):
            for u in range(packs):
                edge_y[pl.ds(u * SUB, SUB), :] = e_new[u][1]
            for u in range(packs):
                i = u * SUB
                rows = pl.ds(i, SUB)
                old = [flat_h[across(c, i + 1, SUB + right), :] for c in range(3)]
                aux = {n: flat_s[within(n, i, right), :] for n in (1, 2, 3, 4)}
                coef_x = [cp[0, n, rows, :] for n in range(3)]
                side_x = (edge_y[pl.ds(i + 1, SUB), :], zero)
                values = (e_new[u], side_x, (zero, zero), old, (), aux, coef_x)
                fields, _f = compute(0, values, None)
                t_ay[0, rows, :] = fields[0]
                t_ay[1, rows, :] = fields[2]

        def sweep(k, count):
            @pl.loop(0, count)
            def _(n):
                unit(k, lax.div(n, tiles), lax.rem(n, tiles))

        def fix_y(s):
            @pl.when(has_hy)
            def _():
                for u in range(packs):
                    i = u * SUB
                    rows = pl.ds(i, SUB)
                    a0, a2 = across(0, i + 1, SUB + right), across(2, i + 1, SUB + right)
                    flat_h[a0, :] = flat_h[a0, :] - half * r_ey[s, 1, rows, :]
                    flat_h[a2, :] = flat_h[a2, :] + half * r_ey[s, 0, rows, :]

            @pl.when(has_ly)
            def _():
                for u in range(packs):
                    i = u * SUB
                    rows = pl.ds(i, SUB)
                    e0, e2 = flat_e[across(0, i, 0), :], flat_e[across(2, i, 0), :]
                    flat_h[across(0, i + 1, SUB - 1), :] = r_ay[s, 0, rows, :] - half * e2
                    flat_h[across(2, i + 1, SUB - 1), :] = r_ay[s, 1, rows, :] + half * e0

        def fix_high(s):
            @pl.when(both(has_hx, has_ly))
            def _():
                edge = pl.ds(SUB - 1, 1)
                H[2, rows_x, edge, :] = (
                    H[2, rows_x, edge, :] - half * r_c1[s, pl.ds(SUB - 1, 1), :]
                )

            @pl.when(has_hx)
            def _():
                H[1, rows_x, inner, :] = H[1, rows_x, inner, :] + half * r_ex[s, 1]
                H[2, rows_x, inner, :] = H[2, rows_x, inner, :] - half * r_ex[s, 0]

        def fix_low(s):
            @pl.when(has_lx)
            def _():
                H[1, 0, inner, :] = r_ax[s, 0] + half * E[2, 0, own, :]
                H[2, 0, inner, :] = r_ax[s, 1] - half * E[1, 0, own, :]

            @pl.when(both(has_lx, has_hy))
            def _():
                edge = pl.ds(SUB + right, 1)
                H[2, 0, edge, :] = H[2, 0, edge, :] + half * r_c0[s, pl.ds(0, 1), :]

        odd = lax.rem(gx, 2) == 1

        def in_turn(high, low):
            @pl.when(odd)
            def _():
                high()
                low()

            @pl.when(jnp.logical_not(odd))
            def _():
                low()
                high()

        count = groups * tiles
        edge_x[pl.ds(rows_y, SUB), :] = zero
        edge_y[pl.ds(rows_x, SUB), :] = zero
        fields_in[0].wait()
        fields_in[1].wait()
        wait_slots(0)
        partial_high([[E[c, top, pl.ds(t * SUB, SUB), :] for c in range(3)] for t in range(tiles)])
        t_ex[0] = E[1, 0, own, :]
        t_ex[1] = E[2, 0, own, :]
        t_c1[...] = E[1, 0, pl.ds(rows_y - SUB, SUB), :]
        partial_y([[flat_e[across(c, u * SUB, right), :] for c in range(3)] for u in range(packs)])
        for u in range(packs):
            i = u * SUB
            rows = pl.ds(i, SUB)
            t_ey[0, rows, :] = flat_e[across(0, i, 0), :]
            t_ey[1, rows, :] = flat_e[across(2, i, 0), :]
        pl.semaphore_wait(barrier, sum(jnp.where(present, 1, 0) for present, _t in links))
        first_high, first_low, first_y = exchange(0)
        in_turn(lambda: start(first_high), lambda: start(first_low))
        start(first_y)
        sweep(0, count)
        fields_in[2].wait()
        materials()
        wait_slots(1)

        def advance(step, carry):
            s = lax.rem(step, 2)
            out_high, out_low, old_y = exchange(s)
            new_high, new_low, new_y = exchange(1 - s)
            arrived(old_y)
            fix_y(s)
            left(old_y)
            left(out_high)
            left(out_low)

            def high():
                arrived(out_low)
                fix_high(s)
                face_high()
                start(new_high)

            def low():
                arrived(out_high)
                fix_low(s)
                face_low()
                start(new_low)

            in_turn(high, low)
            faces_y()
            start(new_y)
            sweep(1, count)
            sweep(0, count)
            return carry

        lax.fori_loop(0, STEPS - 1, advance, 0)
        s = (STEPS - 1) % 2
        last_high, last_low, last_y = exchange(s)
        for moves in (last_y, last_low, last_high):
            arrived(moves)
            left(moves)
        fix_y(s)
        fix_high(s)
        fix_low(s)
        sweep(1, count)

    return kernel


def make_writer(rows_x, rows_y):
    def writer(E, H, S, e_out, h_out, p_out, out_sem):
        outs = [
            pltpu.make_async_copy(
                E.at[:, pl.ds(0, rows_x), pl.ds(0, rows_y), :], e_out, out_sem.at[0]
            ),
            pltpu.make_async_copy(
                H.at[:, pl.ds(1, rows_x), pl.ds(SUB, rows_y), :], h_out, out_sem.at[1]
            ),
            pltpu.make_async_copy(S, p_out, out_sem.at[2]),
        ]
        for c in outs:
            c.start()
        for c in outs:
            c.wait()

    return writer


def solution(mesh):
    size_x, size_y = mesh.shape["gx"], mesh.shape["gy"]

    def shards(e_field, h_field, psi, material, eps_table, sigma_table):
        _, rows_x, rows_y, depth_z = e_field.shape
        assert rows_x == 2 * PML and rows_y == 2 * PML and size_x > 1 and size_y > 1
        f32 = jnp.float32
        any_space = pl.BlockSpec(memory_space=pltpu.HBM)
        smem = pl.BlockSpec(memory_space=pltpu.SMEM)
        face_x = (2, rows_y, depth_z)
        face_y = (2, rows_x, depth_z)
        corner = (SUB, depth_z)
        faces = (face_x, face_y, face_x, face_y, corner, corner)
        padded = (3, rows_x + 1, rows_y + SUB, depth_z)
        cell = (rows_x, rows_y, depth_z)
        vmem = pl.BlockSpec(memory_space=pltpu.VMEM)
        state = pl.pallas_call(
            make_kernel(size_x, size_y, rows_x, rows_y, depth_z),
            out_shape=[pltpu.VMEM(padded, f32), pltpu.VMEM(padded, f32), pltpu.VMEM(psi.shape, f32)],
            in_specs=[any_space] * 4 + [smem] * 2,
            out_specs=[vmem] * 3,
            scratch_shapes=[
                pltpu.VMEM(cell, f32),
                pltpu.VMEM(cell, f32),
                pltpu.VMEM(cell, jnp.int32),
                pltpu.VMEM((2, 3, rows_x, SUB, depth_z), f32),
                pltpu.VMEM((2, 3, rows_y, depth_z), f32),
                pltpu.VMEM((2, 3, rows_x, depth_z), f32),
                pltpu.VMEM((rows_y + SUB, depth_z), f32),
                pltpu.VMEM((rows_x + SUB, depth_z), f32),
            ]
            + [pltpu.VMEM(f, f32) for f in faces]
            + [pltpu.VMEM((2,) + f, f32) for f in faces]
            + [
                pltpu.SemaphoreType.DMA((17,)),
                pltpu.SemaphoreType.DMA((6,)),
                pltpu.SemaphoreType.DMA((6, 2)),
            ],
            compiler_params=pltpu.CompilerParams(
                collective_id=0, has_side_effects=True, vmem_limit_bytes=53 << 20
            ),
        )(e_field, h_field, psi, material, eps_table, sigma_table)
        return pl.pallas_call(
            make_writer(rows_x, rows_y),
            out_shape=[jax.ShapeDtypeStruct(a.shape, f32) for a in (e_field, h_field, psi)],
            in_specs=[vmem] * 3,
            out_specs=[any_space] * 3,
            scratch_shapes=[pltpu.SemaphoreType.DMA((3,))],
            compiler_params=pltpu.CompilerParams(vmem_limit_bytes=24 << 20),
        )(*state)

    split = P(None, "gx", "gy", None)
    return jax.shard_map(
        shards,
        mesh=mesh,
        in_specs=(split, split, split, P("gx", "gy", None), P(), P()),
        out_specs=(split, split, split),
        check_vma=False,
    )
```

```python
import jax
import jax.numpy as jnp
from jax import lax
from jax.experimental import pallas as pl
from jax.experimental.pallas import tpu as pltpu
from jax.sharding import PartitionSpec as P

PML = 16
STEPS = 16
NMAT = 8
SUB = 8
GROUP = 16
AHEAD = 2

time_step = 0.5
sigma_peak = 3.0
kappa_peak = 5.0
alpha_peak = 0.05
MESH = pl.DeviceIdType.MESH


def profile(index, extent, shift_half):
    position = index.astype(jnp.float32) + shift_half
    slab_width = float(PML)
    depth_frac = jnp.maximum(
        jnp.maximum(
            (slab_width - position) / slab_width, (position - (extent - slab_width)) / slab_width
        ),
        0.0,
    )
    depth_cube = depth_frac * depth_frac * depth_frac
    sigma_value = sigma_peak * depth_cube
    kappa_value = 1.0 + (kappa_peak - 1.0) * depth_cube
    alpha_value = alpha_peak * (1.0 - depth_frac)
    decays = jnp.exp(-(sigma_value / kappa_value + alpha_value) * time_step)
    scaling = (
        sigma_value * (decays - 1.0) / (kappa_value * (sigma_value + kappa_value * alpha_value))
    )
    inside_slab = depth_frac > 0.0
    return (
        jnp.where(inside_slab, decays, 0.0),
        jnp.where(inside_slab, scaling, 0.0),
        1.0 / kappa_value,
    )


def make_kernel(size_x, size_y, rows_x, rows_y, depth_z):
    groups = rows_x // GROUP
    tiles = rows_y // SUB
    top, right = rows_x - 1, rows_y - 1

    def kernel(
        e_in, h_in, p_in, m_in, eps_ref, sig_ref, E, H, S,
        keep, drive, mat, cx, cy, cp, edge_x, edge_y,
        t_ex, t_ey, t_ax, t_ay, t_c0, t_c1,
        r_ex, r_ey, r_ax, r_ay, r_c0, r_c1,
        in_sem, send_sem, recv_sem,
    ):
        gx, gy = lax.axis_index("gx"), lax.axis_index("gy")
        has_lx, has_hx = gx > 0, gx < size_x - 1
        has_ly, has_hy = gy > 0, gy < size_y - 1
        slab_x = (gx == 0, gx == size_x - 1)
        slab_y = (gy == 0, gy == size_y - 1)
        lx, hx, ly, hy = gx - 1, gx + 1, gy - 1, gy + 1
        both = jnp.logical_and
        links = (
            (has_lx, (lx, gy)),
            (has_hx, (hx, gy)),
            (has_ly, (gx, ly)),
            (has_hy, (gx, hy)),
            (both(has_hx, has_ly), (hx, ly)),
            (both(has_lx, has_hy), (lx, hy)),
        )

        def field_copies():
            pairs = (
                (e_in, E.at[:, pl.ds(0, rows_x), pl.ds(0, rows_y), :]),
                (h_in, H.at[:, pl.ds(1, rows_x), pl.ds(SUB, rows_y), :]),
                (m_in, mat),
            )
            return [pltpu.make_async_copy(a, b, in_sem.at[n]) for n, (a, b) in enumerate(pairs)]

        def slot_copies(k):
            first, base = 6 * k, 3 + 7 * k
            pair = pl.ds(first + 1, 2)
            always = pltpu.make_async_copy(p_in.at[pair], S.at[pair], in_sem.at[base])
            guarded = []
            for side in (0, 1):
                half_x, pair = pl.ds(side * PML, PML), pl.ds(first + 3, 2)
                guarded.append(
                    (
                        slab_x[side],
                        pltpu.make_async_copy(
                            p_in.at[pair, half_x], S.at[pair, half_x], in_sem.at[base + 1 + side]
                        ),
                    )
                )
                for n, slot in enumerate((first, first + 5)):
                    guarded.append(
                        (
                            slab_y[side],
                            pltpu.make_async_copy(
                                p_in.at[slot, :, half_x],
                                S.at[slot, :, half_x],
                                in_sem.at[base + 3 + 2 * side + n],
                            ),
                        )
                    )
            return always, guarded

        def start_slots(k):
            always, guarded = slot_copies(k)
            always.start()
            for present, copy in guarded:

                @pl.when(present)
                def _():
                    copy.start()

        def wait_slots(k):
            always, guarded = slot_copies(k)
            always.wait()
            for present, copy in guarded:

                @pl.when(present)
                def _():
                    copy.wait()

        fields_in = field_copies()
        fields_in[0].start()
        fields_in[1].start()
        start_slots(0)
        fields_in[2].start()
        start_slots(1)

        barrier = pltpu.get_barrier_semaphore()
        for present, target in links:

            @pl.when(present)
            def _():
                pl.semaphore_signal(barrier, inc=1, device_id=target, device_id_type=MESH)

        zero = jnp.zeros((SUB, depth_z), jnp.float32)
        for side in (0, 1):

            @pl.when(jnp.logical_not(slab_x[side]))
            def _():
                @pl.loop(side * PML, side * PML + PML)
                def _(i):
                    for s in (3, 4, 9, 10):
                        S[s, i] = jnp.zeros((rows_y, depth_z), jnp.float32)

            @pl.when(jnp.logical_not(slab_y[side]))
            def _():
                @pl.loop(0, rows_x)
                def _(i):
                    for s in (0, 5, 6, 11):
                        S[s, i, pl.ds(side * PML, PML), :] = jnp.zeros(
                            (PML, depth_z), jnp.float32
                        )

        for c in range(3):
            for t in range(tiles):
                E[c, rows_x, pl.ds(t * SUB, SUB), :] = zero
                H[c, 0, pl.ds(SUB + t * SUB, SUB), :] = zero

        @pl.loop(0, rows_x)
        def _(i):
            for c in range(3):
                E[c, i, pl.ds(rows_y, SUB), :] = zero
                H[c, i + 1, pl.ds(0, SUB), :] = zero

        lane = lax.broadcasted_iota(jnp.int32, (SUB, depth_z), 1)
        row = lax.broadcasted_iota(jnp.int32, (rows_y, depth_z), 0)
        column = lax.broadcasted_iota(jnp.int32, (rows_x, depth_z), 0)
        plane = lax.broadcasted_iota(jnp.int32, (rows_x, SUB, depth_z), 0)
        zc = []
        for k, shift in enumerate((0.5, 0.0)):
            zc.append(profile(lane, depth_z, shift))
            for n, v in enumerate(profile(row + gy * rows_y, size_y * rows_y, shift)):
                cy[k, n] = v
            for n, v in enumerate(profile(plane + gx * rows_x, size_x * rows_x, shift)):
                cx[k, n] = v
            for n, v in enumerate(profile(column + gx * rows_x, size_x * rows_x, shift)):
                cp[k, n] = v
        not_last = lane < depth_z - 1
        not_first = lane > 0

        def materials():
            keep_vals, drive_vals = [], []
            for m in range(NMAT):
                eps = jnp.full((SUB, depth_z), eps_ref[m], jnp.float32)
                sig = jnp.full((SUB, depth_z), sig_ref[m], jnp.float32)
                loss = sig * time_step / (2.0 * eps)
                keep_vals.append((1.0 - loss) / (1.0 + loss))
                drive_vals.append((time_step / eps) / (1.0 + loss))

            @pl.loop(0, rows_x)
            def _(i):
                for t in range(tiles):
                    rows = pl.ds(t * SUB, SUB)
                    number = mat[i, rows, :]
                    kv, dv = keep_vals[0], drive_vals[0]
                    for m in range(1, NMAT):
                        chosen = number == m
                        kv = jnp.where(chosen, keep_vals[m], kv)
                        dv = jnp.where(chosen, drive_vals[m], dv)
                    keep[i, rows, :] = kv
                    drive[i, rows, :] = dv

        def term(old, d, coef):
            b, a, q = coef
            renewed = b * old + a * d
            return q * d + renewed, renewed

        def loads(k, i, y, in_x, in_y):
            rows, at = pl.ds(y, SUB), pl.ds(y + SUB, SUB)
            first = 6 * k
            if k == 0:
                src, j, now, step, line = E, i, rows, 1, pl.ds(y + 1, SUB)
                old = [H[c, i + 1, at, :] for c in range(3)]
                mats = ()
            else:
                src, j, now, step, line = H, i + 1, at, -1, pl.ds(y + SUB - 1, SUB)
                old = [E[c, i, rows, :] for c in range(3)]
                mats = (keep[i, rows, :], drive[i, rows, :])
            own = [src[c, j, now, :] for c in range(3)]
            side_x = [src[c, j + step, now, :] for c in (1, 2)]
            side_y = [src[c, j, line, :] for c in (0, 2)]
            slots = [1, 2] + ([3, 4] if in_x else []) + ([0, 5] if in_y else [])
            aux = {n: S[first + n, i, rows, :] for n in slots}
            coef_x = [cx[k, n, i] for n in range(3)] if in_x else None
            return own, side_x, side_y, old, mats, aux, coef_x

        def compute(k, values, coef_y):
            own, (x1, x2), (y0, y2), old, mats, aux, coef_x = values
            f0, f1, f2 = own
            if k == 0:
                dx1, dx2, dy0, dy2 = x1 - f1, x2 - f2, y0 - f0, y2 - f2
                dz0 = jnp.where(not_last, pltpu.roll(f0, depth_z - 1, 1), 0.0) - f0
                dz1 = jnp.where(not_last, pltpu.roll(f1, depth_z - 1, 1), 0.0) - f1
            else:
                dx1, dx2, dy0, dy2 = f1 - x1, f2 - x2, f0 - y0, f2 - y2
                dz0 = f0 - jnp.where(not_first, pltpu.roll(f0, 1, 1), 0.0)
                dz1 = f1 - jnp.where(not_first, pltpu.roll(f1, 1, 1), 0.0)
            fresh = {}
            dz1, fresh[1] = term(aux[1], dz1, zc[k])
            dz0, fresh[2] = term(aux[2], dz0, zc[k])
            if coef_x is not None:
                dx2, fresh[3] = term(aux[3], dx2, coef_x)
                dx1, fresh[4] = term(aux[4], dx1, coef_x)
            if coef_y is not None:
                dy2, fresh[0] = term(aux[0], dy2, coef_y)
                dy0, fresh[5] = term(aux[5], dy0, coef_y)
            curls = (dy2 - dz1, dz0 - dx2, dx1 - dy0)
            if k == 0:
                return [o - time_step * c for o, c in zip(old, curls)], fresh
            return [mats[0] * o + mats[1] * c for o, c in zip(old, curls)], fresh

        def stores(k, i, y, result):
            fields, fresh = result
            for c in range(3):
                if k == 0:
                    H[c, i + 1, pl.ds(y + SUB, SUB), :] = fields[c]
                else:
                    E[c, i, pl.ds(y, SUB), :] = fields[c]
            for n, v in fresh.items():
                S[6 * k + n, i, pl.ds(y, SUB), :] = v

        def run(k, i0, y, in_x, in_y):
            coef_y = [cy[k, n, pl.ds(y, SUB), :] for n in range(3)] if in_y else None
            ready = [loads(k, i0 + u, y, in_x, in_y) for u in range(AHEAD)]
            for u in range(GROUP):
                if u + AHEAD < GROUP:
                    ready.append(loads(k, i0 + u + AHEAD, y, in_x, in_y))
                stores(k, i0 + u, y, compute(k, ready[u], coef_y))

        def unit(k, g, t):
            low_x, low_y = g * GROUP < PML, t * SUB < PML
            px = jnp.where(low_x, slab_x[0], slab_x[1])
            py = jnp.where(low_y, slab_y[0], slab_y[1])
            i0, y = g * GROUP, pl.multiple_of(t * SUB, SUB)

            def split_y(in_x):
                lax.cond(
                    py,
                    lambda: run(k, i0, y, in_x, True),
                    lambda: run(k, i0, y, in_x, False),
                )

            lax.cond(px, lambda: split_y(True), lambda: split_y(False))

        def exchange(s):
            one, last = pl.ds(0, 1), pl.ds(SUB - 1, 1)
            diag_c0, diag_c1 = both(has_hx, has_ly), both(has_lx, has_hy)
            moves = (
                (diag_c0, (hx, ly), diag_c1, t_c0.at[one], r_c0.at[s, one]),
                (has_hx, (hx, gy), has_lx, t_ax.at[1], r_ax.at[s, 1]),
                (has_hx, (hx, gy), has_lx, t_ax.at[0], r_ax.at[s, 0]),
                (diag_c1, (lx, hy), diag_c0, t_c1.at[last], r_c1.at[s, last]),
                (has_lx, (lx, gy), has_hx, t_ex.at[0], r_ex.at[s, 0]),
                (has_lx, (lx, gy), has_hx, t_ex.at[1], r_ex.at[s, 1]),
                (has_ly, (gx, ly), has_hy, t_ey, r_ey.at[s]),
                (has_hy, (gx, hy), has_ly, t_ay, r_ay.at[s]),
            )
            made = [
                (
                    sends,
                    gets,
                    pltpu.make_async_remote_copy(
                        src_ref=src,
                        dst_ref=dst,
                        send_sem=send_sem.at[n],
                        recv_sem=recv_sem.at[n, s],
                        device_id=target,
                        device_id_type=MESH,
                    ),
                )
                for n, (sends, target, gets, src, dst) in enumerate(moves)
            ]
            return made[:3], made[3:6], made[6:]

        own = pl.ds(0, rows_y)
        inner = pl.ds(SUB, rows_y)
        half = time_step
        wide = rows_y + SUB
        flat_e = E.reshape(3 * (rows_x + 1) * wide, depth_z)
        flat_h = H.reshape(3 * (rows_x + 1) * wide, depth_z)
        flat_s = S.reshape(12 * rows_x * rows_y, depth_z)
        flat_keep = keep.reshape(rows_x * rows_y, depth_z)
        flat_drive = drive.reshape(rows_x * rows_y, depth_z)
        packs = rows_x // SUB

        def across(c, i, y):
            return pl.ds((c * (rows_x + 1) + i) * wide + y, SUB, stride=wide)

        def within(c, i, y):
            return pl.ds((c * rows_x + i) * rows_y + y, SUB, stride=rows_y)

        def start(moves):
            for sends, _g, copy in moves:

                @pl.when(sends)
                def _():
                    copy.start()

        def arrived(moves):
            for _s, gets, copy in moves:

                @pl.when(gets)
                def _():
                    copy.wait_recv()

        def left(moves):
            for sends, _g, copy in moves:

                @pl.when(sends)
                def _():
                    copy.wait_send()

        def coefs_y(k, y):
            return [cy[k, n, pl.ds(y, SUB), :] for n in range(3)]

        def face_low(c):
            for t in range(tiles):
                y = t * SUB
                fields, _f = compute(1, loads(1, 0, y, False, True), coefs_y(1, y))
                t_ex[c - 1, pl.ds(y, SUB), :] = fields[c]
                if c == 1 and t == tiles - 1:
                    t_c1[...] = fields[1]

        def face_high():
            fields = []
            for t in range(tiles):
                y = t * SUB
                fields.append(compute(1, loads(1, top, y, False, True), coefs_y(1, y))[0])
            t_c0[...] = fields[0][0]
            for t in range(tiles):
                rows = pl.ds(t * SUB, SUB)
                edge_x[0, rows, :] = fields[t][0]
                edge_x[1, rows, :] = fields[t][1]
                edge_x[2, rows, :] = fields[t][2]

        def partial_high(c):
            for t in range(tiles):
                y = t * SUB
                rows, at = pl.ds(y, SUB), pl.ds(y + SUB, SUB)
                e_new = [edge_x[n, rows, :] for n in range(3)]
                old = [H[n, rows_x, at, :] for n in range(3)]
                aux = {n: S[n, top, rows, :] for n in (1, 2, 0, 5)}
                side_y = (edge_x[0, pl.ds(y + 1, SUB), :], zero)
                values = (e_new, (zero, zero), side_y, old, (), aux, None)
                fields, _f = compute(0, values, coefs_y(0, y))
                t_ax[c - 1, rows, :] = fields[c]

        def packed_e(r, u):
            i = u * SUB
            own_h = [flat_h[across(c, i + 1, SUB + r), :] for c in range(3)]
            side_x = [flat_h[across(c, i, SUB + r), :] for c in (1, 2)]
            side_y = [flat_h[across(c, i + 1, SUB + r - 1), :] for c in (0, 2)]
            old = [flat_e[across(c, i, r), :] for c in range(3)]
            mats = (flat_keep[within(0, i, r), :], flat_drive[within(0, i, r), :])
            aux = {n: flat_s[within(6 + n, i, r), :] for n in (1, 2, 3, 4)}
            coef_x = [cp[1, n, pl.ds(i, SUB), :] for n in range(3)]
            return compute(1, (own_h, side_x, side_y, old, mats, aux, coef_x), None)[0]

        def faces_y():
            late = []
            for u in range(packs):
                rows = pl.ds(u * SUB, SUB)
                fields = packed_e(0, u)
                t_ey[0, rows, :] = fields[0]
                t_ey[1, rows, :] = fields[2]
                late.append(packed_e(right, u))
            partial_y(late)

        def partial_y(e_new):
            for u in range(packs):
                edge_y[pl.ds(u * SUB, SUB), :] = e_new[u][1]
            for u in range(packs):
                i = u * SUB
                rows = pl.ds(i, SUB)
                old = [flat_h[across(c, i + 1, SUB + right), :] for c in range(3)]
                aux = {n: flat_s[within(n, i, right), :] for n in (1, 2, 3, 4)}
                coef_x = [cp[0, n, rows, :] for n in range(3)]
                side_x = (edge_y[pl.ds(i + 1, SUB), :], zero)
                values = (e_new[u], side_x, (zero, zero), old, (), aux, coef_x)
                fields, _f = compute(0, values, None)
                t_ay[0, rows, :] = fields[0]
                t_ay[1, rows, :] = fields[2]

        def sweep(k, count):
            @pl.loop(0, count)
            def _(n):
                unit(k, lax.div(n, tiles), lax.rem(n, tiles))

        def fix_y(s):
            @pl.when(has_hy)
            def _():
                for u in range(packs):
                    i = u * SUB
                    rows = pl.ds(i, SUB)
                    a0, a2 = across(0, i + 1, SUB + right), across(2, i + 1, SUB + right)
                    flat_h[a0, :] = flat_h[a0, :] - half * r_ey[s, 1, rows, :]
                    flat_h[a2, :] = flat_h[a2, :] + half * r_ey[s, 0, rows, :]

            @pl.when(has_ly)
            def _():
                for u in range(packs):
                    i = u * SUB
                    rows = pl.ds(i, SUB)
                    e0, e2 = flat_e[across(0, i, 0), :], flat_e[across(2, i, 0), :]
                    flat_h[across(0, i + 1, SUB - 1), :] = r_ay[s, 0, rows, :] - half * e2
                    flat_h[across(2, i + 1, SUB - 1), :] = r_ay[s, 1, rows, :] + half * e0

        def fix_high(s):
            @pl.when(both(has_hx, has_ly))
            def _():
                edge = pl.ds(SUB - 1, 1)
                H[2, rows_x, edge, :] = (
                    H[2, rows_x, edge, :] - half * r_c1[s, pl.ds(SUB - 1, 1), :]
                )

            @pl.when(has_hx)
            def _():
                H[1, rows_x, inner, :] = H[1, rows_x, inner, :] + half * r_ex[s, 1]
                H[2, rows_x, inner, :] = H[2, rows_x, inner, :] - half * r_ex[s, 0]

        def fix_low_2(s):
            @pl.when(has_lx)
            def _():
                H[2, 0, inner, :] = r_ax[s, 1] - half * E[1, 0, own, :]

            @pl.when(both(has_lx, has_hy))
            def _():
                edge = pl.ds(SUB + right, 1)
                H[2, 0, edge, :] = H[2, 0, edge, :] + half * r_c0[s, pl.ds(0, 1), :]

        def fix_low_1(s):
            @pl.when(has_lx)
            def _():
                H[1, 0, inner, :] = r_ax[s, 0] + half * E[2, 0, own, :]

        odd = lax.rem(gx, 2) == 1

        def in_turn(high, low):
            @pl.when(odd)
            def _():
                high()
                low()

            @pl.when(jnp.logical_not(odd))
            def _():
                low()
                high()

        count = groups * tiles
        edge_x[0, pl.ds(rows_y, SUB), :] = zero
        edge_y[pl.ds(rows_x, SUB), :] = zero
        fields_in[0].wait()
        fields_in[1].wait()
        wait_slots(0)
        t_c0[...] = E[0, top, pl.ds(0, SUB), :]
        for c in range(3):
            edge_x[c, own, :] = E[c, top, own, :]
        partial_high(2)
        partial_high(1)
        t_ex[0] = E[1, 0, own, :]
        t_ex[1] = E[2, 0, own, :]
        t_c1[...] = E[1, 0, pl.ds(rows_y - SUB, SUB), :]
        partial_y([[flat_e[across(c, u * SUB, right), :] for c in range(3)] for u in range(packs)])
        for u in range(packs):
            i = u * SUB
            rows = pl.ds(i, SUB)
            t_ey[0, rows, :] = flat_e[across(0, i, 0), :]
            t_ey[1, rows, :] = flat_e[across(2, i, 0), :]
        pl.semaphore_wait(barrier, sum(jnp.where(present, 1, 0) for present, _t in links))
        first_high, first_low, first_y = exchange(0)
        in_turn(lambda: start(first_high), lambda: start(first_low))
        start(first_y)
        sweep(0, count)
        fields_in[2].wait()
        materials()
        wait_slots(1)

        def advance(step, carry):
            s = lax.rem(step, 2)
            out_high, out_low, old_y = exchange(s)
            new_high, new_low, new_y = exchange(1 - s)
            arrived(old_y)
            fix_y(s)
            left(old_y)
            left(out_high)
            left(out_low)

            def high():
                arrived(out_low)
                fix_high(s)
                face_high()
                partial_high(2)
                start(new_high[:2])
                partial_high(1)
                start(new_high[2:])

            def low():
                arrived(out_high[:2])
                fix_low_2(s)
                face_low(1)
                start(new_low[:2])
                arrived(out_high[2:])
                fix_low_1(s)
                face_low(2)
                start(new_low[2:])

            in_turn(high, low)
            faces_y()
            start(new_y)
            sweep(1, count)
            sweep(0, count)
            return carry

        lax.fori_loop(0, STEPS - 1, advance, 0)
        s = (STEPS - 1) % 2
        last_high, last_low, last_y = exchange(s)
        for moves in (last_y, last_low, last_high):
            arrived(moves)
            left(moves)
        fix_y(s)
        fix_high(s)
        fix_low_2(s)
        fix_low_1(s)
        sweep(1, count)

    return kernel


def make_writer(rows_x, rows_y):
    def writer(E, H, S, e_out, h_out, p_out, out_sem):
        outs = [
            pltpu.make_async_copy(
                E.at[:, pl.ds(0, rows_x), pl.ds(0, rows_y), :], e_out, out_sem.at[0]
            ),
            pltpu.make_async_copy(
                H.at[:, pl.ds(1, rows_x), pl.ds(SUB, rows_y), :], h_out, out_sem.at[1]
            ),
            pltpu.make_async_copy(S, p_out, out_sem.at[2]),
        ]
        for c in outs:
            c.start()
        for c in outs:
            c.wait()

    return writer


def solution(mesh):
    size_x, size_y = mesh.shape["gx"], mesh.shape["gy"]

    def shards(e_field, h_field, psi, material, eps_table, sigma_table):
        _, rows_x, rows_y, depth_z = e_field.shape
        assert rows_x == 2 * PML and rows_y == 2 * PML and size_x > 1 and size_y > 1
        f32 = jnp.float32
        any_space = pl.BlockSpec(memory_space=pltpu.HBM)
        smem = pl.BlockSpec(memory_space=pltpu.SMEM)
        face_x = (2, rows_y, depth_z)
        face_y = (2, rows_x, depth_z)
        corner = (SUB, depth_z)
        faces = (face_x, face_y, face_x, face_y, corner, corner)
        padded = (3, rows_x + 1, rows_y + SUB, depth_z)
        cell = (rows_x, rows_y, depth_z)
        vmem = pl.BlockSpec(memory_space=pltpu.VMEM)
        state = pl.pallas_call(
            make_kernel(size_x, size_y, rows_x, rows_y, depth_z),
            out_shape=[pltpu.VMEM(padded, f32), pltpu.VMEM(padded, f32), pltpu.VMEM(psi.shape, f32)],
            in_specs=[any_space] * 4 + [smem] * 2,
            out_specs=[vmem] * 3,
            scratch_shapes=[
                pltpu.VMEM(cell, f32),
                pltpu.VMEM(cell, f32),
                pltpu.VMEM(cell, jnp.int32),
                pltpu.VMEM((2, 3, rows_x, SUB, depth_z), f32),
                pltpu.VMEM((2, 3, rows_y, depth_z), f32),
                pltpu.VMEM((2, 3, rows_x, depth_z), f32),
                pltpu.VMEM((3, rows_y + SUB, depth_z), f32),
                pltpu.VMEM((rows_x + SUB, depth_z), f32),
            ]
            + [pltpu.VMEM(f, f32) for f in faces]
            + [pltpu.VMEM((2,) + f, f32) for f in faces]
            + [
                pltpu.SemaphoreType.DMA((17,)),
                pltpu.SemaphoreType.DMA((8,)),
                pltpu.SemaphoreType.DMA((8, 2)),
            ],
            compiler_params=pltpu.CompilerParams(
                collective_id=0, has_side_effects=True, vmem_limit_bytes=53 << 20
            ),
        )(e_field, h_field, psi, material, eps_table, sigma_table)
        return pl.pallas_call(
            make_writer(rows_x, rows_y),
            out_shape=[jax.ShapeDtypeStruct(a.shape, f32) for a in (e_field, h_field, psi)],
            in_specs=[vmem] * 3,
            out_specs=[any_space] * 3,
            scratch_shapes=[pltpu.SemaphoreType.DMA((3,))],
            compiler_params=pltpu.CompilerParams(vmem_limit_bytes=24 << 20),
        )(*state)

    split = P(None, "gx", "gy", None)
    return jax.shard_map(
        shards,
        mesh=mesh,
        in_specs=(split, split, split, P("gx", "gy", None), P(), P()),
        out_specs=(split, split, split),
        check_vma=False,
    )
```

```python
import jax
import jax.numpy as jnp
from jax import lax
from jax.experimental import pallas as pl
from jax.experimental.pallas import tpu as pltpu
from jax.sharding import PartitionSpec as P

PML = 16
STEPS = 16
NMAT = 8
SUB = 8
GROUP = 16
AHEAD = 2

time_step = 0.5
sigma_peak = 3.0
kappa_peak = 5.0
alpha_peak = 0.05
MESH = pl.DeviceIdType.MESH


def profile(index, extent, shift_half):
    position = index.astype(jnp.float32) + shift_half
    slab_width = float(PML)
    depth_frac = jnp.maximum(
        jnp.maximum(
            (slab_width - position) / slab_width, (position - (extent - slab_width)) / slab_width
        ),
        0.0,
    )
    depth_cube = depth_frac * depth_frac * depth_frac
    sigma_value = sigma_peak * depth_cube
    kappa_value = 1.0 + (kappa_peak - 1.0) * depth_cube
    alpha_value = alpha_peak * (1.0 - depth_frac)
    decays = jnp.exp(-(sigma_value / kappa_value + alpha_value) * time_step)
    scaling = (
        sigma_value * (decays - 1.0) / (kappa_value * (sigma_value + kappa_value * alpha_value))
    )
    inside_slab = depth_frac > 0.0
    return (
        jnp.where(inside_slab, decays, 0.0),
        jnp.where(inside_slab, scaling, 0.0),
        1.0 / kappa_value,
    )


def make_cell(
    E, H, S, keep, drive, cx, cy, zc, slab_x, slab_y, tiles, depth_z, e_to, s_to, s_base
):
    lane = lax.broadcasted_iota(jnp.int32, (SUB, depth_z), 1)
    not_last = lane < depth_z - 1
    not_first = lane > 0

    def term(old, d, coef):
        b, a, q = coef
        renewed = b * old + a * d
        return q * d + renewed, renewed

    def loads(k, i, y, in_x, in_y):
        rows, at = pl.ds(y, SUB), pl.ds(y + SUB, SUB)
        first = 6 * k
        if k == 0:
            src, j, now, step, line = E, i, rows, 1, pl.ds(y + 1, SUB)
            old = [H[c, i + 1, at, :] for c in range(3)]
            mats = ()
        else:
            src, j, now, step, line = H, i + 1, at, -1, pl.ds(y + SUB - 1, SUB)
            old = [E[c, i, rows, :] for c in range(3)]
            mats = (keep[i, rows, :], drive[i, rows, :])
        own = [src[c, j, now, :] for c in range(3)]
        side_x = [src[c, j + step, now, :] for c in (1, 2)]
        side_y = [src[c, j, line, :] for c in (0, 2)]
        slots = [1, 2] + ([3, 4] if in_x else []) + ([0, 5] if in_y else [])
        aux = {n: S[first + n, i, rows, :] for n in slots}
        coef_x = [cx[k, n, i] for n in range(3)] if in_x else None
        return own, side_x, side_y, old, mats, aux, coef_x

    def compute(k, values, coef_y):
        own, (x1, x2), (y0, y2), old, mats, aux, coef_x = values
        f0, f1, f2 = own
        if k == 0:
            dx1, dx2, dy0, dy2 = x1 - f1, x2 - f2, y0 - f0, y2 - f2
            dz0 = jnp.where(not_last, pltpu.roll(f0, depth_z - 1, 1), 0.0) - f0
            dz1 = jnp.where(not_last, pltpu.roll(f1, depth_z - 1, 1), 0.0) - f1
        else:
            dx1, dx2, dy0, dy2 = f1 - x1, f2 - x2, f0 - y0, f2 - y2
            dz0 = f0 - jnp.where(not_first, pltpu.roll(f0, 1, 1), 0.0)
            dz1 = f1 - jnp.where(not_first, pltpu.roll(f1, 1, 1), 0.0)
        fresh = {}
        dz1, fresh[1] = term(aux[1], dz1, zc[k])
        dz0, fresh[2] = term(aux[2], dz0, zc[k])
        if coef_x is not None:
            dx2, fresh[3] = term(aux[3], dx2, coef_x)
            dx1, fresh[4] = term(aux[4], dx1, coef_x)
        if coef_y is not None:
            dy2, fresh[0] = term(aux[0], dy2, coef_y)
            dy0, fresh[5] = term(aux[5], dy0, coef_y)
        curls = (dy2 - dz1, dz0 - dx2, dx1 - dy0)
        if k == 0:
            return [o - time_step * c for o, c in zip(old, curls)], fresh
        return [mats[0] * o + mats[1] * c for o, c in zip(old, curls)], fresh

    def stores(k, i, y, result):
        fields, fresh = result
        for c in range(3):
            if k == 0:
                H[c, i + 1, pl.ds(y + SUB, SUB), :] = fields[c]
            else:
                e_to[c, i, pl.ds(y, SUB), :] = fields[c]
        for n, v in fresh.items():
            s_to[6 * k + n - s_base, i, pl.ds(y, SUB), :] = v

    def run(k, i0, y, in_x, in_y):
        coef_y = [cy[k, n, pl.ds(y, SUB), :] for n in range(3)] if in_y else None
        ready = [loads(k, i0 + u, y, in_x, in_y) for u in range(AHEAD)]
        for u in range(GROUP):
            if u + AHEAD < GROUP:
                ready.append(loads(k, i0 + u + AHEAD, y, in_x, in_y))
            stores(k, i0 + u, y, compute(k, ready[u], coef_y))

    def unit(k, g, t):
        low_x, low_y = g * GROUP < PML, t * SUB < PML
        px = jnp.where(low_x, slab_x[0], slab_x[1])
        py = jnp.where(low_y, slab_y[0], slab_y[1])
        i0, y = g * GROUP, pl.multiple_of(t * SUB, SUB)

        def split_y(in_x):
            lax.cond(
                py,
                lambda: run(k, i0, y, in_x, True),
                lambda: run(k, i0, y, in_x, False),
            )

        lax.cond(px, lambda: split_y(True), lambda: split_y(False))

    return loads, compute, unit


def make_kernel(size_x, size_y, rows_x, rows_y, depth_z):
    groups = rows_x // GROUP
    tiles = rows_y // SUB
    top, right = rows_x - 1, rows_y - 1

    def kernel(
        e_in, h_in, p_in, m_in, eps_ref, sig_ref, E, H, S,
        keep, drive, cx, cy, mat, cp, edge_x, edge_y,
        t_ex, t_ey, t_ax, t_ay, t_c0, t_c1,
        r_ex, r_ey, r_ax, r_ay, r_c0, r_c1,
        in_sem, send_sem, recv_sem,
    ):
        gx, gy = lax.axis_index("gx"), lax.axis_index("gy")
        has_lx, has_hx = gx > 0, gx < size_x - 1
        has_ly, has_hy = gy > 0, gy < size_y - 1
        slab_x = (gx == 0, gx == size_x - 1)
        slab_y = (gy == 0, gy == size_y - 1)
        lx, hx, ly, hy = gx - 1, gx + 1, gy - 1, gy + 1
        both = jnp.logical_and
        links = (
            (has_lx, (lx, gy)),
            (has_hx, (hx, gy)),
            (has_ly, (gx, ly)),
            (has_hy, (gx, hy)),
            (both(has_hx, has_ly), (hx, ly)),
            (both(has_lx, has_hy), (lx, hy)),
        )

        mid = pl.ds(0, rows_y)

        def e_copy(first, number, n):
            layers = pl.ds(first, number)
            return pltpu.make_async_copy(e_in.at[:, layers], E.at[:, layers, mid, :], in_sem.at[n])

        def h_copy(first, number, n):
            return pltpu.make_async_copy(
                h_in.at[:, pl.ds(first, number)],
                H.at[:, pl.ds(first + 1, number), pl.ds(SUB, rows_y), :],
                in_sem.at[n],
            )

        def slot_copies(k, first, number, n):
            layers, pair = pl.ds(first, number), pl.ds(6 * k + 1, 2)
            made = [
                (
                    None,
                    pltpu.make_async_copy(
                        p_in.at[pair, layers], S.at[pair, layers], in_sem.at[n]
                    ),
                )
            ]
            for side in (0, 1):
                rows = pl.ds(side * PML, PML)
                for j, slot in enumerate((6 * k, 6 * k + 5)):
                    made.append(
                        (
                            slab_y[side],
                            pltpu.make_async_copy(
                                p_in.at[slot, layers, rows],
                                S.at[slot, layers, rows],
                                in_sem.at[n + 1 + 2 * side + j],
                            ),
                        )
                    )
            return made

        def across_copies(k, n):
            pair = pl.ds(6 * k + 3, 2)
            made = []
            for side in (0, 1):
                layers = pl.ds(side * PML, PML)
                made.append(
                    (
                        slab_x[side],
                        pltpu.make_async_copy(
                            p_in.at[pair, layers], S.at[pair, layers], in_sem.at[n + side]
                        ),
                    )
                )
            return made

        def each(copies, act):
            for present, copy in copies:
                if present is None:
                    act(copy)
                else:

                    @pl.when(present)
                    def _():
                        act(copy)

        def begin(copies):
            each(copies, lambda copy: copy.start())

        def settle(copies):
            each(copies, lambda copy: copy.wait())

        rim = [(None, e_copy(top, 1, 0)), (None, h_copy(top, 1, 1))]
        rim += slot_copies(0, top, 1, 2) + [(None, e_copy(0, 1, 7))]
        rest = [(None, e_copy(1, top - 1, 8)), (None, h_copy(0, top, 9))]
        rest += slot_copies(0, 0, top, 10) + across_copies(0, 15)
        kinds = [(None, pltpu.make_async_copy(m_in, mat, in_sem.at[17]))]
        later = slot_copies(1, 0, rows_x, 18) + across_copies(1, 23)
        for copies in (rim, rest, kinds, later):
            begin(copies)

        barrier = pltpu.get_barrier_semaphore()
        for present, target in links:

            @pl.when(present)
            def _():
                pl.semaphore_signal(barrier, inc=1, device_id=target, device_id_type=MESH)

        zero = jnp.zeros((SUB, depth_z), jnp.float32)
        for side in (0, 1):

            @pl.when(jnp.logical_not(slab_y[side]))
            def _():
                @pl.loop(0, rows_x)
                def _(i):
                    for s in (0, 5, 6, 11):
                        S[s, i, pl.ds(side * PML, PML), :] = jnp.zeros(
                            (PML, depth_z), jnp.float32
                        )

        lane = lax.broadcasted_iota(jnp.int32, (SUB, depth_z), 1)
        row = lax.broadcasted_iota(jnp.int32, (rows_y, depth_z), 0)
        zc = []
        for k, shift in enumerate((0.5, 0.0)):
            zc.append(profile(lane, depth_z, shift))
            for n, v in enumerate(profile(row + gy * rows_y, size_y * rows_y, shift)):
                cy[k, n] = v

        def clear_rest():
            for side in (0, 1):

                @pl.when(jnp.logical_not(slab_x[side]))
                def _():
                    @pl.loop(side * PML, side * PML + PML)
                    def _(i):
                        for s in (3, 4, 9, 10):
                            S[s, i] = jnp.zeros((rows_y, depth_z), jnp.float32)

            for c in range(3):
                for t in range(tiles):
                    E[c, rows_x, pl.ds(t * SUB, SUB), :] = zero
                    H[c, 0, pl.ds(SUB + t * SUB, SUB), :] = zero

            @pl.loop(0, rows_x)
            def _(i):
                for c in range(3):
                    E[c, i, pl.ds(rows_y, SUB), :] = zero
                    H[c, i + 1, pl.ds(0, SUB), :] = zero

            column = lax.broadcasted_iota(jnp.int32, (rows_x, depth_z), 0)
            plane = lax.broadcasted_iota(jnp.int32, (rows_x, SUB, depth_z), 0)
            for k, shift in enumerate((0.5, 0.0)):
                for n, v in enumerate(profile(plane + gx * rows_x, size_x * rows_x, shift)):
                    cx[k, n] = v
                for n, v in enumerate(profile(column + gx * rows_x, size_x * rows_x, shift)):
                    cp[k, n] = v

        def materials():
            keep_vals, drive_vals = [], []
            for m in range(NMAT):
                eps = jnp.full((SUB, depth_z), eps_ref[m], jnp.float32)
                sig = jnp.full((SUB, depth_z), sig_ref[m], jnp.float32)
                loss = sig * time_step / (2.0 * eps)
                keep_vals.append((1.0 - loss) / (1.0 + loss))
                drive_vals.append((time_step / eps) / (1.0 + loss))

            @pl.loop(0, rows_x)
            def _(i):
                for t in range(tiles):
                    rows = pl.ds(t * SUB, SUB)
                    number = mat[i, rows, :]
                    kv, dv = keep_vals[0], drive_vals[0]
                    for m in range(1, NMAT):
                        chosen = number == m
                        kv = jnp.where(chosen, keep_vals[m], kv)
                        dv = jnp.where(chosen, drive_vals[m], dv)
                    keep[i, rows, :] = kv
                    drive[i, rows, :] = dv

        loads, compute, unit = make_cell(
            E, H, S, keep, drive, cx, cy, zc, slab_x, slab_y, tiles, depth_z, E, S, 0
        )

        def exchange(s):
            one, last = pl.ds(0, 1), pl.ds(SUB - 1, 1)
            diag_c0, diag_c1 = both(has_hx, has_ly), both(has_lx, has_hy)
            moves = (
                (diag_c0, (hx, ly), diag_c1, t_c0.at[one], r_c0.at[s, one]),
                (has_hx, (hx, gy), has_lx, t_ax.at[1], r_ax.at[s, 1]),
                (has_hx, (hx, gy), has_lx, t_ax.at[0], r_ax.at[s, 0]),
                (diag_c1, (lx, hy), diag_c0, t_c1.at[last], r_c1.at[s, last]),
                (has_lx, (lx, gy), has_hx, t_ex.at[0], r_ex.at[s, 0]),
                (has_lx, (lx, gy), has_hx, t_ex.at[1], r_ex.at[s, 1]),
                (has_ly, (gx, ly), has_hy, t_ey, r_ey.at[s]),
                (has_hy, (gx, hy), has_ly, t_ay, r_ay.at[s]),
            )
            made = [
                (
                    sends,
                    gets,
                    pltpu.make_async_remote_copy(
                        src_ref=src,
                        dst_ref=dst,
                        send_sem=send_sem.at[n],
                        recv_sem=recv_sem.at[n, s],
                        device_id=target,
                        device_id_type=MESH,
                    ),
                )
                for n, (sends, target, gets, src, dst) in enumerate(moves)
            ]
            return made[:3], made[3:6], made[6:]

        own = pl.ds(0, rows_y)
        inner = pl.ds(SUB, rows_y)
        half = time_step
        wide = rows_y + SUB
        flat_e = E.reshape(3 * (rows_x + 1) * wide, depth_z)
        flat_h = H.reshape(3 * (rows_x + 1) * wide, depth_z)
        flat_s = S.reshape(12 * rows_x * rows_y, depth_z)
        flat_keep = keep.reshape(rows_x * rows_y, depth_z)
        flat_drive = drive.reshape(rows_x * rows_y, depth_z)
        packs = rows_x // SUB

        def across(c, i, y):
            return pl.ds((c * (rows_x + 1) + i) * wide + y, SUB, stride=wide)

        def within(c, i, y):
            return pl.ds((c * rows_x + i) * rows_y + y, SUB, stride=rows_y)

        def start(moves):
            for sends, _g, copy in moves:

                @pl.when(sends)
                def _():
                    copy.start()

        def arrived(moves):
            for _s, gets, copy in moves:

                @pl.when(gets)
                def _():
                    copy.wait_recv()

        def left(moves):
            for sends, _g, copy in moves:

                @pl.when(sends)
                def _():
                    copy.wait_send()

        def coefs_y(k, y):
            return [cy[k, n, pl.ds(y, SUB), :] for n in range(3)]

        def face_low(c):
            for t in range(tiles):
                y = t * SUB
                fields, _f = compute(1, loads(1, 0, y, False, True), coefs_y(1, y))
                t_ex[c - 1, pl.ds(y, SUB), :] = fields[c]
                if c == 1 and t == tiles - 1:
                    t_c1[...] = fields[1]

        def face_high():
            fields = []
            for t in range(tiles):
                y = t * SUB
                fields.append(compute(1, loads(1, top, y, False, True), coefs_y(1, y))[0])
            t_c0[...] = fields[0][0]
            for t in range(tiles):
                rows = pl.ds(t * SUB, SUB)
                edge_x[0, rows, :] = fields[t][0]
                edge_x[1, rows, :] = fields[t][1]
                edge_x[2, rows, :] = fields[t][2]

        def partial_high(c):
            for t in range(tiles):
                y = t * SUB
                rows, at = pl.ds(y, SUB), pl.ds(y + SUB, SUB)
                e_new = [edge_x[n, rows, :] for n in range(3)]
                old = [H[n, rows_x, at, :] for n in range(3)]
                aux = {n: S[n, top, rows, :] for n in (1, 2, 0, 5)}
                side_y = (edge_x[0, pl.ds(y + 1, SUB), :], zero)
                values = (e_new, (zero, zero), side_y, old, (), aux, None)
                fields, _f = compute(0, values, coefs_y(0, y))
                t_ax[c - 1, rows, :] = fields[c]

        def packed_e(r, u):
            i = u * SUB
            own_h = [flat_h[across(c, i + 1, SUB + r), :] for c in range(3)]
            side_x = [flat_h[across(c, i, SUB + r), :] for c in (1, 2)]
            side_y = [flat_h[across(c, i + 1, SUB + r - 1), :] for c in (0, 2)]
            old = [flat_e[across(c, i, r), :] for c in range(3)]
            mats = (flat_keep[within(0, i, r), :], flat_drive[within(0, i, r), :])
            aux = {n: flat_s[within(6 + n, i, r), :] for n in (1, 2, 3, 4)}
            coef_x = [cp[1, n, pl.ds(i, SUB), :] for n in range(3)]
            return compute(1, (own_h, side_x, side_y, old, mats, aux, coef_x), None)[0]

        def faces_y():
            late = []
            for u in range(packs):
                rows = pl.ds(u * SUB, SUB)
                fields = packed_e(0, u)
                t_ey[0, rows, :] = fields[0]
                t_ey[1, rows, :] = fields[2]
                late.append(packed_e(right, u))
            partial_y(late)

        def partial_y(e_new):
            for u in range(packs):
                edge_y[pl.ds(u * SUB, SUB), :] = e_new[u][1]
            for u in range(packs):
                i = u * SUB
                rows = pl.ds(i, SUB)
                old = [flat_h[across(c, i + 1, SUB + right), :] for c in range(3)]
                aux = {n: flat_s[within(n, i, right), :] for n in (1, 2, 3, 4)}
                coef_x = [cp[0, n, rows, :] for n in range(3)]
                side_x = (edge_y[pl.ds(i + 1, SUB), :], zero)
                values = (e_new[u], side_x, (zero, zero), old, (), aux, coef_x)
                fields, _f = compute(0, values, None)
                t_ay[0, rows, :] = fields[0]
                t_ay[1, rows, :] = fields[2]

        def sweep(k, count):
            @pl.loop(0, count)
            def _(n):
                unit(k, lax.div(n, tiles), lax.rem(n, tiles))

        def fix_y(s):
            @pl.when(has_hy)
            def _():
                for u in range(packs):
                    i = u * SUB
                    rows = pl.ds(i, SUB)
                    a0, a2 = across(0, i + 1, SUB + right), across(2, i + 1, SUB + right)
                    flat_h[a0, :] = flat_h[a0, :] - half * r_ey[s, 1, rows, :]
                    flat_h[a2, :] = flat_h[a2, :] + half * r_ey[s, 0, rows, :]

            @pl.when(has_ly)
            def _():
                for u in range(packs):
                    i = u * SUB
                    rows = pl.ds(i, SUB)
                    e0, e2 = flat_e[across(0, i, 0), :], flat_e[across(2, i, 0), :]
                    flat_h[across(0, i + 1, SUB - 1), :] = r_ay[s, 0, rows, :] - half * e2
                    flat_h[across(2, i + 1, SUB - 1), :] = r_ay[s, 1, rows, :] + half * e0

        def fix_high(s):
            @pl.when(both(has_hx, has_ly))
            def _():
                edge = pl.ds(SUB - 1, 1)
                H[2, rows_x, edge, :] = (
                    H[2, rows_x, edge, :] - half * r_c1[s, pl.ds(SUB - 1, 1), :]
                )

            @pl.when(has_hx)
            def _():
                H[1, rows_x, inner, :] = H[1, rows_x, inner, :] + half * r_ex[s, 1]
                H[2, rows_x, inner, :] = H[2, rows_x, inner, :] - half * r_ex[s, 0]

        def fix_low_2(s):
            @pl.when(has_lx)
            def _():
                H[2, 0, inner, :] = r_ax[s, 1] - half * E[1, 0, own, :]

            @pl.when(both(has_lx, has_hy))
            def _():
                edge = pl.ds(SUB + right, 1)
                H[2, 0, edge, :] = H[2, 0, edge, :] + half * r_c0[s, pl.ds(0, 1), :]

        def fix_low_1(s):
            @pl.when(has_lx)
            def _():
                H[1, 0, inner, :] = r_ax[s, 0] + half * E[2, 0, own, :]

        odd = lax.rem(gx, 2) == 1

        def in_turn(high, low):
            @pl.when(odd)
            def _():
                high()
                low()

            @pl.when(jnp.logical_not(odd))
            def _():
                low()
                high()

        count = groups * tiles
        edge_x[0, pl.ds(rows_y, SUB), :] = zero
        edge_y[pl.ds(rows_x, SUB), :] = zero
        settle(rim)
        t_c0[...] = E[0, top, pl.ds(0, SUB), :]
        for c in range(3):
            edge_x[c, own, :] = E[c, top, own, :]
        partial_high(2)
        partial_high(1)
        t_ex[0] = E[1, 0, own, :]
        t_ex[1] = E[2, 0, own, :]
        t_c1[...] = E[1, 0, pl.ds(rows_y - SUB, SUB), :]
        pl.semaphore_wait(barrier, sum(jnp.where(present, 1, 0) for present, _t in links))
        first_high, first_low, first_y = exchange(0)
        in_turn(lambda: start(first_high), lambda: start(first_low))
        clear_rest()
        settle(rest)
        partial_y([[flat_e[across(c, u * SUB, right), :] for c in range(3)] for u in range(packs)])
        for u in range(packs):
            i = u * SUB
            rows = pl.ds(i, SUB)
            t_ey[0, rows, :] = flat_e[across(0, i, 0), :]
            t_ey[1, rows, :] = flat_e[across(2, i, 0), :]
        start(first_y)
        sweep(0, count)
        settle(kinds)
        materials()
        settle(later)

        def advance(step, carry):
            s = lax.rem(step, 2)
            out_high, out_low, old_y = exchange(s)
            new_high, new_low, new_y = exchange(1 - s)
            arrived(old_y)
            fix_y(s)
            left(old_y)
            left(out_high)
            left(out_low)

            def high():
                arrived(out_low)
                fix_high(s)
                face_high()
                partial_high(2)
                start(new_high[:2])
                partial_high(1)
                start(new_high[2:])

            def low():
                arrived(out_high[:2])
                fix_low_2(s)
                face_low(1)
                start(new_low[:2])
                arrived(out_high[2:])
                fix_low_1(s)
                face_low(2)
                start(new_low[2:])

            in_turn(high, low)
            faces_y()
            start(new_y)
            sweep(1, count)
            sweep(0, count)
            return carry

        lax.fori_loop(0, STEPS - 1, advance, 0)
        s = (STEPS - 1) % 2
        last_high, last_low, last_y = exchange(s)
        for moves in (last_y, last_low, last_high):
            arrived(moves)
            left(moves)
        fix_y(s)
        fix_high(s)
        fix_low_2(s)
        fix_low_1(s)

    return kernel


def make_writer(size_x, size_y, rows_x, rows_y, depth_z):
    groups = rows_x // GROUP
    tiles = rows_y // SUB

    def writer(E, H, S, keep, drive, cx, cy, e_out, h_out, p_out, e_new, s_new, out_sem):
        gx, gy = lax.axis_index("gx"), lax.axis_index("gy")
        slab_x = (gx == 0, gx == size_x - 1)
        slab_y = (gy == 0, gy == size_y - 1)
        copy = pltpu.make_async_copy
        h_part = copy(H.at[:, pl.ds(1, rows_x), pl.ds(SUB, rows_y), :], h_out, out_sem.at[0])
        p_part = copy(S.at[pl.ds(0, 6)], p_out.at[pl.ds(0, 6)], out_sem.at[1])
        h_part.start()
        p_part.start()
        slabs = []
        for side in (0, 1):
            half, pair = pl.ds(side * PML, PML), pl.ds(9, 2)
            to, sem = p_out.at[pair, half], out_sem.at[2 + side]
            early = copy(S.at[pair, half], to, sem)
            slabs.append((slab_x[side], early, copy(s_new.at[pl.ds(3, 2), half], to, sem)))
            for j, slot in enumerate((6, 11)):
                to, sem = p_out.at[slot, :, half], out_sem.at[4 + 2 * side + j]
                early = copy(S.at[slot, :, half], to, sem)
                slabs.append((slab_y[side], early, copy(s_new.at[slot - 6, :, half], to, sem)))
        for inside, early, _late in slabs:

            @pl.when(jnp.logical_not(inside))
            def _():
                early.start()

        zc = [profile(lax.broadcasted_iota(jnp.int32, (SUB, depth_z), 1), depth_z, 0.0)] * 2
        _loads, _compute, unit = make_cell(
            E, H, S, keep, drive, cx, cy, zc, slab_x, slab_y, tiles, depth_z, e_new, s_new, 6
        )
        made = []
        for g in range(groups):
            layers, pair, one_two = pl.ds(g * GROUP, GROUP), pl.ds(7, 2), pl.ds(1, 2)
            made.append(
                [
                    copy(e_new.at[:, layers], e_out.at[:, layers], out_sem.at[8 + 2 * g]),
                    copy(s_new.at[one_two, layers], p_out.at[pair, layers], out_sem.at[9 + 2 * g]),
                ]
            )

            @pl.loop(0, tiles)
            def _(t):
                unit(1, g, t)

            if g > 0:
                for c in made[g - 1]:
                    c.start()
        h_part.wait()
        for c in made[-1]:
            c.start()
        for inside, _early, late in slabs:

            @pl.when(inside)
            def _():
                late.start()

        p_part.wait()
        for _inside, early, _late in slabs:
            early.wait()
        for pieces in made:
            for c in pieces:
                c.wait()

    return writer


def solution(mesh):
    size_x, size_y = mesh.shape["gx"], mesh.shape["gy"]

    def shards(e_field, h_field, psi, material, eps_table, sigma_table):
        _, rows_x, rows_y, depth_z = e_field.shape
        assert rows_x == 2 * PML and rows_y == 2 * PML and size_x > 1 and size_y > 1
        f32 = jnp.float32
        any_space = pl.BlockSpec(memory_space=pltpu.HBM)
        smem = pl.BlockSpec(memory_space=pltpu.SMEM)
        face_x = (2, rows_y, depth_z)
        face_y = (2, rows_x, depth_z)
        corner = (SUB, depth_z)
        faces = (face_x, face_y, face_x, face_y, corner, corner)
        padded = (3, rows_x + 1, rows_y + SUB, depth_z)
        cell = (rows_x, rows_y, depth_z)
        vmem = pl.BlockSpec(memory_space=pltpu.VMEM)
        strip = (2, 3, rows_x, SUB, depth_z)
        edge = (2, 3, rows_y, depth_z)
        held = (padded, padded, psi.shape, cell, cell, strip, edge)
        state = pl.pallas_call(
            make_kernel(size_x, size_y, rows_x, rows_y, depth_z),
            out_shape=[pltpu.VMEM(shape, f32) for shape in held],
            in_specs=[any_space] * 4 + [smem] * 2,
            out_specs=[vmem] * len(held),
            scratch_shapes=[
                pltpu.VMEM(cell, jnp.int32),
                pltpu.VMEM((2, 3, rows_x, depth_z), f32),
                pltpu.VMEM((3, rows_y + SUB, depth_z), f32),
                pltpu.VMEM((rows_x + SUB, depth_z), f32),
            ]
            + [pltpu.VMEM(f, f32) for f in faces]
            + [pltpu.VMEM((2,) + f, f32) for f in faces]
            + [
                pltpu.SemaphoreType.DMA((25,)),
                pltpu.SemaphoreType.DMA((8,)),
                pltpu.SemaphoreType.DMA((8, 2)),
            ],
            compiler_params=pltpu.CompilerParams(
                collective_id=0, has_side_effects=True, vmem_limit_bytes=48 << 20
            ),
        )(e_field, h_field, psi, material, eps_table, sigma_table)
        return pl.pallas_call(
            make_writer(size_x, size_y, rows_x, rows_y, depth_z),
            out_shape=[jax.ShapeDtypeStruct(a.shape, f32) for a in (e_field, h_field, psi)],
            in_specs=[vmem] * len(held),
            out_specs=[any_space] * 3,
            scratch_shapes=[
                pltpu.VMEM((3,) + cell, f32),
                pltpu.VMEM((6,) + cell, f32),
                pltpu.SemaphoreType.DMA((8 + 2 * (rows_x // GROUP),)),
            ],
            compiler_params=pltpu.CompilerParams(vmem_limit_bytes=32 << 20),
        )(*state)

    split = P(None, "gx", "gy", None)
    return jax.shard_map(
        shards,
        mesh=mesh,
        in_specs=(split, split, split, P("gx", "gy", None), P(), P()),
        out_specs=(split, split, split),
        check_vma=False,
    )
```

```python
import jax
import jax.numpy as jnp
from jax import lax
from jax.experimental import pallas as pl
from jax.experimental.pallas import tpu as pltpu
from jax.sharding import PartitionSpec as P

PML = 16
STEPS = 16
NMAT = 8
SUB = 8
GROUP = 16
AHEAD = 2

time_step = 0.5
sigma_peak = 3.0
kappa_peak = 5.0
alpha_peak = 0.05
MESH = pl.DeviceIdType.MESH


def profile(index, extent, shift_half):
    position = index.astype(jnp.float32) + shift_half
    slab_width = float(PML)
    depth_frac = jnp.maximum(
        jnp.maximum(
            (slab_width - position) / slab_width, (position - (extent - slab_width)) / slab_width
        ),
        0.0,
    )
    depth_cube = depth_frac * depth_frac * depth_frac
    sigma_value = sigma_peak * depth_cube
    kappa_value = 1.0 + (kappa_peak - 1.0) * depth_cube
    alpha_value = alpha_peak * (1.0 - depth_frac)
    decays = jnp.exp(-(sigma_value / kappa_value + alpha_value) * time_step)
    scaling = (
        sigma_value * (decays - 1.0) / (kappa_value * (sigma_value + kappa_value * alpha_value))
    )
    inside_slab = depth_frac > 0.0
    return (
        jnp.where(inside_slab, decays, 0.0),
        jnp.where(inside_slab, scaling, 0.0),
        1.0 / kappa_value,
    )


def make_cell(
    E, H, S, keep, drive, cx, cy, zc, slab_x, slab_y, tiles, depth_z, e_to, s_to, s_base
):
    lane = lax.broadcasted_iota(jnp.int32, (SUB, depth_z), 1)
    not_last = lane < depth_z - 1
    not_first = lane > 0

    def term(old, d, coef):
        b, a, q = coef
        renewed = b * old + a * d
        return q * d + renewed, renewed

    def loads(k, i, y, in_x, in_y):
        rows, at = pl.ds(y, SUB), pl.ds(y + SUB, SUB)
        first = 6 * k
        if k == 0:
            src, j, now, step, line = E, i, rows, 1, pl.ds(y + 1, SUB)
            old = [H[c, i + 1, at, :] for c in range(3)]
            mats = ()
        else:
            src, j, now, step, line = H, i + 1, at, -1, pl.ds(y + SUB - 1, SUB)
            old = [E[c, i, rows, :] for c in range(3)]
            mats = (keep[i, rows, :], drive[i, rows, :])
        own = [src[c, j, now, :] for c in range(3)]
        side_x = [src[c, j + step, now, :] for c in (1, 2)]
        side_y = [src[c, j, line, :] for c in (0, 2)]
        slots = [1, 2] + ([3, 4] if in_x else []) + ([0, 5] if in_y else [])
        aux = {n: S[first + n, i, rows, :] for n in slots}
        coef_x = [cx[k, n, i] for n in range(3)] if in_x else None
        return own, side_x, side_y, old, mats, aux, coef_x

    def compute(k, values, coef_y):
        own, (x1, x2), (y0, y2), old, mats, aux, coef_x = values
        f0, f1, f2 = own
        if k == 0:
            dx1, dx2, dy0, dy2 = x1 - f1, x2 - f2, y0 - f0, y2 - f2
            dz0 = jnp.where(not_last, pltpu.roll(f0, depth_z - 1, 1), 0.0) - f0
            dz1 = jnp.where(not_last, pltpu.roll(f1, depth_z - 1, 1), 0.0) - f1
        else:
            dx1, dx2, dy0, dy2 = f1 - x1, f2 - x2, f0 - y0, f2 - y2
            dz0 = f0 - jnp.where(not_first, pltpu.roll(f0, 1, 1), 0.0)
            dz1 = f1 - jnp.where(not_first, pltpu.roll(f1, 1, 1), 0.0)
        fresh = {}
        dz1, fresh[1] = term(aux[1], dz1, zc[k])
        dz0, fresh[2] = term(aux[2], dz0, zc[k])
        if coef_x is not None:
            dx2, fresh[3] = term(aux[3], dx2, coef_x)
            dx1, fresh[4] = term(aux[4], dx1, coef_x)
        if coef_y is not None:
            dy2, fresh[0] = term(aux[0], dy2, coef_y)
            dy0, fresh[5] = term(aux[5], dy0, coef_y)
        curls = (dy2 - dz1, dz0 - dx2, dx1 - dy0)
        if k == 0:
            return [o - time_step * c for o, c in zip(old, curls)], fresh
        return [mats[0] * o + mats[1] * c for o, c in zip(old, curls)], fresh

    def stores(k, i, y, result):
        fields, fresh = result
        for c in range(3):
            if k == 0:
                H[c, i + 1, pl.ds(y + SUB, SUB), :] = fields[c]
            else:
                e_to[c, i, pl.ds(y, SUB), :] = fields[c]
        for n, v in fresh.items():
            s_to[6 * k + n - s_base, i, pl.ds(y, SUB), :] = v

    def run(k, i0, y, in_x, in_y):
        coef_y = [cy[k, n, pl.ds(y, SUB), :] for n in range(3)] if in_y else None
        ready = [loads(k, i0 + u, y, in_x, in_y) for u in range(AHEAD)]
        for u in range(GROUP):
            if u + AHEAD < GROUP:
                ready.append(loads(k, i0 + u + AHEAD, y, in_x, in_y))
            stores(k, i0 + u, y, compute(k, ready[u], coef_y))

    def unit(k, g, t):
        low_x, low_y = g * GROUP < PML, t * SUB < PML
        px = jnp.where(low_x, slab_x[0], slab_x[1])
        py = jnp.where(low_y, slab_y[0], slab_y[1])
        i0, y = g * GROUP, pl.multiple_of(t * SUB, SUB)

        def split_y(in_x):
            lax.cond(
                py,
                lambda: run(k, i0, y, in_x, True),
                lambda: run(k, i0, y, in_x, False),
            )

        lax.cond(px, lambda: split_y(True), lambda: split_y(False))

    return loads, compute, unit


def make_kernel(size_x, size_y, rows_x, rows_y, depth_z):
    groups = rows_x // GROUP
    tiles = rows_y // SUB
    top, right = rows_x - 1, rows_y - 1

    def kernel(
        e_in, h_in, p_in, m_in, eps_ref, sig_ref, E, H, S,
        keep, drive, cx, cy, mat, cp, edge_x, edge_y,
        t_ex, t_ey, t_ax, t_ay, t_c0, t_c1,
        r_ex, r_ey, r_ax, r_ay, r_c0, r_c1,
        in_sem, send_sem, recv_sem,
    ):
        gx, gy = lax.axis_index("gx"), lax.axis_index("gy")
        has_lx, has_hx = gx > 0, gx < size_x - 1
        has_ly, has_hy = gy > 0, gy < size_y - 1
        slab_x = (gx == 0, gx == size_x - 1)
        slab_y = (gy == 0, gy == size_y - 1)
        lx, hx, ly, hy = gx - 1, gx + 1, gy - 1, gy + 1
        both = jnp.logical_and
        links = (
            (has_lx, (lx, gy)),
            (has_hx, (hx, gy)),
            (has_ly, (gx, ly)),
            (has_hy, (gx, hy)),
            (both(has_hx, has_ly), (hx, ly)),
            (both(has_lx, has_hy), (lx, hy)),
        )

        barrier = pltpu.get_barrier_semaphore()
        for present, target in links:

            @pl.when(present)
            def _():
                pl.semaphore_signal(barrier, inc=1, device_id=target, device_id_type=MESH)

        mid = pl.ds(0, rows_y)

        def e_copy(first, number, n):
            layers = pl.ds(first, number)
            return pltpu.make_async_copy(e_in.at[:, layers], E.at[:, layers, mid, :], in_sem.at[n])

        def h_copy(first, number, n):
            return pltpu.make_async_copy(
                h_in.at[:, pl.ds(first, number)],
                H.at[:, pl.ds(first + 1, number), pl.ds(SUB, rows_y), :],
                in_sem.at[n],
            )

        def slot_copies(k, first, number, n):
            layers, pair = pl.ds(first, number), pl.ds(6 * k + 1, 2)
            made = [
                (
                    None,
                    pltpu.make_async_copy(
                        p_in.at[pair, layers], S.at[pair, layers], in_sem.at[n]
                    ),
                )
            ]
            for side in (0, 1):
                rows = pl.ds(side * PML, PML)
                for j, slot in enumerate((6 * k, 6 * k + 5)):
                    made.append(
                        (
                            slab_y[side],
                            pltpu.make_async_copy(
                                p_in.at[slot, layers, rows],
                                S.at[slot, layers, rows],
                                in_sem.at[n + 1 + 2 * side + j],
                            ),
                        )
                    )
            return made

        def across_copies(k, n):
            pair = pl.ds(6 * k + 3, 2)
            made = []
            for side in (0, 1):
                layers = pl.ds(side * PML, PML)
                made.append(
                    (
                        slab_x[side],
                        pltpu.make_async_copy(
                            p_in.at[pair, layers], S.at[pair, layers], in_sem.at[n + side]
                        ),
                    )
                )
            return made

        def each(copies, act):
            for present, copy in copies:
                if present is None:
                    act(copy)
                else:

                    @pl.when(present)
                    def _():
                        act(copy)

        def begin(copies):
            each(copies, lambda copy: copy.start())

        def settle(copies):
            each(copies, lambda copy: copy.wait())

        rim = [(None, e_copy(top, 1, 0)), (None, h_copy(top, 1, 1))]
        rim += slot_copies(0, top, 1, 2) + [(None, e_copy(0, 1, 7))]
        rest = [(None, e_copy(1, top - 1, 8)), (None, h_copy(0, top, 9))]
        rest += slot_copies(0, 0, top, 10) + across_copies(0, 15)
        kinds = [(None, pltpu.make_async_copy(m_in, mat, in_sem.at[17]))]
        later = slot_copies(1, 0, rows_x, 18) + across_copies(1, 23)
        for copies in (rim, rest, kinds, later):
            begin(copies)

        zero = jnp.zeros((SUB, depth_z), jnp.float32)
        for side in (0, 1):

            @pl.when(jnp.logical_not(slab_y[side]))
            def _():
                @pl.loop(0, rows_x)
                def _(i):
                    for s in (0, 5, 6, 11):
                        S[s, i, pl.ds(side * PML, PML), :] = jnp.zeros(
                            (PML, depth_z), jnp.float32
                        )

        lane = lax.broadcasted_iota(jnp.int32, (SUB, depth_z), 1)
        row = lax.broadcasted_iota(jnp.int32, (rows_y, depth_z), 0)
        zc = []
        for k, shift in enumerate((0.5, 0.0)):
            zc.append(profile(lane, depth_z, shift))
            for n, v in enumerate(profile(row + gy * rows_y, size_y * rows_y, shift)):
                cy[k, n] = v

        def clear_rest():
            for side in (0, 1):

                @pl.when(jnp.logical_not(slab_x[side]))
                def _():
                    @pl.loop(side * PML, side * PML + PML)
                    def _(i):
                        for s in (3, 4, 9, 10):
                            S[s, i] = jnp.zeros((rows_y, depth_z), jnp.float32)

            for c in range(3):
                for t in range(tiles):
                    E[c, rows_x, pl.ds(t * SUB, SUB), :] = zero
                    H[c, 0, pl.ds(SUB + t * SUB, SUB), :] = zero

            @pl.loop(0, rows_x)
            def _(i):
                for c in range(3):
                    E[c, i, pl.ds(rows_y, SUB), :] = zero
                    H[c, i + 1, pl.ds(0, SUB), :] = zero

            column = lax.broadcasted_iota(jnp.int32, (rows_x, depth_z), 0)
            plane = lax.broadcasted_iota(jnp.int32, (rows_x, SUB, depth_z), 0)
            for k, shift in enumerate((0.5, 0.0)):
                for n, v in enumerate(profile(plane + gx * rows_x, size_x * rows_x, shift)):
                    cx[k, n] = v
                for n, v in enumerate(profile(column + gx * rows_x, size_x * rows_x, shift)):
                    cp[k, n] = v

        def materials():
            keep_vals, drive_vals = [], []
            for m in range(NMAT):
                eps = jnp.full((SUB, depth_z), eps_ref[m], jnp.float32)
                sig = jnp.full((SUB, depth_z), sig_ref[m], jnp.float32)
                loss = sig * time_step / (2.0 * eps)
                keep_vals.append((1.0 - loss) / (1.0 + loss))
                drive_vals.append((time_step / eps) / (1.0 + loss))

            @pl.loop(0, rows_x)
            def _(i):
                for t in range(tiles):
                    rows = pl.ds(t * SUB, SUB)
                    number = mat[i, rows, :]
                    kv, dv = keep_vals[0], drive_vals[0]
                    for m in range(1, NMAT):
                        chosen = number == m
                        kv = jnp.where(chosen, keep_vals[m], kv)
                        dv = jnp.where(chosen, drive_vals[m], dv)
                    keep[i, rows, :] = kv
                    drive[i, rows, :] = dv

        loads, compute, unit = make_cell(
            E, H, S, keep, drive, cx, cy, zc, slab_x, slab_y, tiles, depth_z, E, S, 0
        )

        def exchange(s):
            one, last = pl.ds(0, 1), pl.ds(SUB - 1, 1)
            diag_c0, diag_c1 = both(has_hx, has_ly), both(has_lx, has_hy)
            moves = (
                (diag_c0, (hx, ly), diag_c1, t_c0.at[one], r_c0.at[s, one]),
                (has_hx, (hx, gy), has_lx, t_ax.at[1], r_ax.at[s, 1]),
                (has_hx, (hx, gy), has_lx, t_ax.at[0], r_ax.at[s, 0]),
                (diag_c1, (lx, hy), diag_c0, t_c1.at[last], r_c1.at[s, last]),
                (has_lx, (lx, gy), has_hx, t_ex.at[0], r_ex.at[s, 0]),
                (has_lx, (lx, gy), has_hx, t_ex.at[1], r_ex.at[s, 1]),
                (has_ly, (gx, ly), has_hy, t_ey, r_ey.at[s]),
                (has_hy, (gx, hy), has_ly, t_ay, r_ay.at[s]),
            )
            made = [
                (
                    sends,
                    gets,
                    pltpu.make_async_remote_copy(
                        src_ref=src,
                        dst_ref=dst,
                        send_sem=send_sem.at[n],
                        recv_sem=recv_sem.at[n, s],
                        device_id=target,
                        device_id_type=MESH,
                    ),
                )
                for n, (sends, target, gets, src, dst) in enumerate(moves)
            ]
            return made[:3], made[3:6], made[6:]

        own = pl.ds(0, rows_y)
        inner = pl.ds(SUB, rows_y)
        half = time_step
        wide = rows_y + SUB
        flat_e = E.reshape(3 * (rows_x + 1) * wide, depth_z)
        flat_h = H.reshape(3 * (rows_x + 1) * wide, depth_z)
        flat_s = S.reshape(12 * rows_x * rows_y, depth_z)
        flat_keep = keep.reshape(rows_x * rows_y, depth_z)
        flat_drive = drive.reshape(rows_x * rows_y, depth_z)
        packs = rows_x // SUB

        def across(c, i, y):
            return pl.ds((c * (rows_x + 1) + i) * wide + y, SUB, stride=wide)

        def within(c, i, y):
            return pl.ds((c * rows_x + i) * rows_y + y, SUB, stride=rows_y)

        def start(moves):
            for sends, _g, copy in moves:

                @pl.when(sends)
                def _():
                    copy.start()

        def arrived(moves):
            for _s, gets, copy in moves:

                @pl.when(gets)
                def _():
                    copy.wait_recv()

        def left(moves):
            for sends, _g, copy in moves:

                @pl.when(sends)
                def _():
                    copy.wait_send()

        def coefs_y(k, y):
            return [cy[k, n, pl.ds(y, SUB), :] for n in range(3)]

        def face_low(c):
            for t in range(tiles):
                y = t * SUB
                fields, _f = compute(1, loads(1, 0, y, False, True), coefs_y(1, y))
                t_ex[c - 1, pl.ds(y, SUB), :] = fields[c]
                if c == 1 and t == tiles - 1:
                    t_c1[...] = fields[1]

        def face_high():
            fields = []
            for t in range(tiles):
                y = t * SUB
                fields.append(compute(1, loads(1, top, y, False, True), coefs_y(1, y))[0])
            t_c0[...] = fields[0][0]
            for t in range(tiles):
                rows = pl.ds(t * SUB, SUB)
                edge_x[0, rows, :] = fields[t][0]
                edge_x[1, rows, :] = fields[t][1]
                edge_x[2, rows, :] = fields[t][2]

        def partial_high(c):
            for t in range(tiles):
                y = t * SUB
                rows, at = pl.ds(y, SUB), pl.ds(y + SUB, SUB)
                e_new = [edge_x[n, rows, :] for n in range(3)]
                old = [H[n, rows_x, at, :] for n in range(3)]
                aux = {n: S[n, top, rows, :] for n in (1, 2, 0, 5)}
                side_y = (edge_x[0, pl.ds(y + 1, SUB), :], zero)
                values = (e_new, (zero, zero), side_y, old, (), aux, None)
                fields, _f = compute(0, values, coefs_y(0, y))
                t_ax[c - 1, rows, :] = fields[c]

        def packed_e(r, u):
            i = u * SUB
            own_h = [flat_h[across(c, i + 1, SUB + r), :] for c in range(3)]
            side_x = [flat_h[across(c, i, SUB + r), :] for c in (1, 2)]
            side_y = [flat_h[across(c, i + 1, SUB + r - 1), :] for c in (0, 2)]
            old = [flat_e[across(c, i, r), :] for c in range(3)]
            mats = (flat_keep[within(0, i, r), :], flat_drive[within(0, i, r), :])
            aux = {n: flat_s[within(6 + n, i, r), :] for n in (1, 2, 3, 4)}
            coef_x = [cp[1, n, pl.ds(i, SUB), :] for n in range(3)]
            return compute(1, (own_h, side_x, side_y, old, mats, aux, coef_x), None)[0]

        def faces_y():
            late = []
            for u in range(packs):
                rows = pl.ds(u * SUB, SUB)
                fields = packed_e(0, u)
                t_ey[0, rows, :] = fields[0]
                t_ey[1, rows, :] = fields[2]
                late.append(packed_e(right, u))
            partial_y(late)

        def partial_y(e_new):
            for u in range(packs):
                edge_y[pl.ds(u * SUB, SUB), :] = e_new[u][1]
            for u in range(packs):
                i = u * SUB
                rows = pl.ds(i, SUB)
                old = [flat_h[across(c, i + 1, SUB + right), :] for c in range(3)]
                aux = {n: flat_s[within(n, i, right), :] for n in (1, 2, 3, 4)}
                coef_x = [cp[0, n, rows, :] for n in range(3)]
                side_x = (edge_y[pl.ds(i + 1, SUB), :], zero)
                values = (e_new[u], side_x, (zero, zero), old, (), aux, coef_x)
                fields, _f = compute(0, values, None)
                t_ay[0, rows, :] = fields[0]
                t_ay[1, rows, :] = fields[2]

        def sweep(k, count):
            @pl.loop(0, count)
            def _(n):
                unit(k, lax.div(n, tiles), lax.rem(n, tiles))

        def fix_y(s):
            @pl.when(has_hy)
            def _():
                for u in range(packs):
                    i = u * SUB
                    rows = pl.ds(i, SUB)
                    a0, a2 = across(0, i + 1, SUB + right), across(2, i + 1, SUB + right)
                    flat_h[a0, :] = flat_h[a0, :] - half * r_ey[s, 1, rows, :]
                    flat_h[a2, :] = flat_h[a2, :] + half * r_ey[s, 0, rows, :]

            @pl.when(has_ly)
            def _():
                for u in range(packs):
                    i = u * SUB
                    rows = pl.ds(i, SUB)
                    e0, e2 = flat_e[across(0, i, 0), :], flat_e[across(2, i, 0), :]
                    flat_h[across(0, i + 1, SUB - 1), :] = r_ay[s, 0, rows, :] - half * e2
                    flat_h[across(2, i + 1, SUB - 1), :] = r_ay[s, 1, rows, :] + half * e0

        def fix_corner_high(s):
            edge = pl.ds(SUB - 1, 1)
            H[2, rows_x, edge, :] = H[2, rows_x, edge, :] - half * r_c1[s, pl.ds(SUB - 1, 1), :]

        def fix_high(s):
            H[1, rows_x, inner, :] = H[1, rows_x, inner, :] + half * r_ex[s, 1]
            H[2, rows_x, inner, :] = H[2, rows_x, inner, :] - half * r_ex[s, 0]

        def fix_low_2(s):
            H[2, 0, inner, :] = r_ax[s, 1] - half * E[1, 0, own, :]

        def fix_corner_low(s):
            edge = pl.ds(SUB + right, 1)
            H[2, 0, edge, :] = H[2, 0, edge, :] + half * r_c0[s, pl.ds(0, 1), :]

        def fix_low_1(s):
            H[1, 0, inner, :] = r_ax[s, 0] + half * E[2, 0, own, :]

        def when(present, act):
            @pl.when(present)
            def _():
                act()

        def arrive_high(s, came):
            corner, first, second = [copy for _s, _g, copy in came]

            @pl.when(has_ly)
            def _():
                corner.wait_recv()
                fix_corner_high(s)

            first.wait_recv()
            second.wait_recv()
            fix_high(s)

        def arrive_low_2(s, came):
            corner, first, _second = [copy for _s, _g, copy in came]
            first.wait_recv()
            fix_low_2(s)

            @pl.when(has_hy)
            def _():
                corner.wait_recv()
                fix_corner_low(s)

        def arrive_low_1(s, came):
            came[2][2].wait_recv()
            fix_low_1(s)

        odd = lax.rem(gx, 2) == 1

        def in_turn(high, low):
            when(both(odd, has_hx), high)
            when(has_lx, low)
            when(both(jnp.logical_not(odd), has_hx), high)

        count = groups * tiles
        edge_x[0, pl.ds(rows_y, SUB), :] = zero
        edge_y[pl.ds(rows_x, SUB), :] = zero
        settle(rim)
        t_c0[...] = E[0, top, pl.ds(0, SUB), :]
        for c in range(3):
            edge_x[c, own, :] = E[c, top, own, :]
        partial_high(2)
        partial_high(1)
        t_ex[0] = E[1, 0, own, :]
        t_ex[1] = E[2, 0, own, :]
        t_c1[...] = E[1, 0, pl.ds(rows_y - SUB, SUB), :]
        pl.semaphore_wait(barrier, sum(jnp.where(present, 1, 0) for present, _t in links))
        first_high, first_low, first_y = exchange(0)
        in_turn(lambda: start(first_high), lambda: start(first_low))
        clear_rest()
        settle(rest)
        partial_y([[flat_e[across(c, u * SUB, right), :] for c in range(3)] for u in range(packs)])
        for u in range(packs):
            i = u * SUB
            rows = pl.ds(i, SUB)
            t_ey[0, rows, :] = flat_e[across(0, i, 0), :]
            t_ey[1, rows, :] = flat_e[across(2, i, 0), :]
        start(first_y)
        sweep(0, count)
        settle(kinds)
        materials()
        settle(later)

        def advance(step, carry):
            s = lax.rem(step, 2)
            out_high, out_low, old_y = exchange(s)
            new_high, new_low, new_y = exchange(1 - s)
            arrived(old_y)
            fix_y(s)
            left(old_y)
            left(out_high)
            left(out_low)

            def high():
                corner, first, second = [copy for _s, _g, copy in new_high]
                arrive_high(s, out_low)
                face_high()
                partial_high(2)
                when(has_ly, corner.start)
                first.start()
                partial_high(1)
                second.start()

            def low():
                corner, first, second = [copy for _s, _g, copy in new_low]
                arrive_low_2(s, out_high)
                face_low(1)
                when(has_hy, corner.start)
                first.start()
                arrive_low_1(s, out_high)
                face_low(2)
                second.start()

            in_turn(high, low)
            faces_y()
            start(new_y)
            sweep(1, count)
            sweep(0, count)
            return carry

        lax.fori_loop(0, STEPS - 1, advance, 0)
        s = (STEPS - 1) % 2
        last_high, last_low, last_y = exchange(s)
        arrived(last_y)
        fix_y(s)

        def last_from_low():
            arrive_low_2(s, last_high)
            arrive_low_1(s, last_high)

        when(has_hx, lambda: arrive_high(s, last_low))
        when(has_lx, last_from_low)
        for moves in (last_y, last_low, last_high):
            left(moves)

    return kernel


def make_writer(size_x, size_y, rows_x, rows_y, depth_z):
    groups = rows_x // GROUP
    tiles = rows_y // SUB

    def writer(E, H, S, keep, drive, cx, cy, e_out, h_out, p_out, e_new, s_new, out_sem):
        gx, gy = lax.axis_index("gx"), lax.axis_index("gy")
        slab_x = (gx == 0, gx == size_x - 1)
        slab_y = (gy == 0, gy == size_y - 1)
        copy = pltpu.make_async_copy
        h_part = copy(H.at[:, pl.ds(1, rows_x), pl.ds(SUB, rows_y), :], h_out, out_sem.at[0])
        p_part = copy(S.at[pl.ds(0, 6)], p_out.at[pl.ds(0, 6)], out_sem.at[1])
        h_part.start()
        p_part.start()
        slabs = []
        for side in (0, 1):
            half, pair = pl.ds(side * PML, PML), pl.ds(9, 2)
            to, sem = p_out.at[pair, half], out_sem.at[2 + side]
            early = copy(S.at[pair, half], to, sem)
            slabs.append((slab_x[side], early, copy(s_new.at[pl.ds(3, 2), half], to, sem)))
            for j, slot in enumerate((6, 11)):
                to, sem = p_out.at[slot, :, half], out_sem.at[4 + 2 * side + j]
                early = copy(S.at[slot, :, half], to, sem)
                slabs.append((slab_y[side], early, copy(s_new.at[slot - 6, :, half], to, sem)))
        for inside, early, _late in slabs:

            @pl.when(jnp.logical_not(inside))
            def _():
                early.start()

        zc = [profile(lax.broadcasted_iota(jnp.int32, (SUB, depth_z), 1), depth_z, 0.0)] * 2
        _loads, _compute, unit = make_cell(
            E, H, S, keep, drive, cx, cy, zc, slab_x, slab_y, tiles, depth_z, e_new, s_new, 6
        )
        made = []
        for g in range(groups):
            layers, pair, one_two = pl.ds(g * GROUP, GROUP), pl.ds(7, 2), pl.ds(1, 2)
            made.append(
                [
                    copy(e_new.at[:, layers], e_out.at[:, layers], out_sem.at[8 + 2 * g]),
                    copy(s_new.at[one_two, layers], p_out.at[pair, layers], out_sem.at[9 + 2 * g]),
                ]
            )

            @pl.loop(0, tiles)
            def _(t):
                unit(1, g, t)

            if g > 0:
                for c in made[g - 1]:
                    c.start()
        h_part.wait()
        for c in made[-1]:
            c.start()
        for inside, _early, late in slabs:

            @pl.when(inside)
            def _():
                late.start()

        p_part.wait()
        for _inside, early, _late in slabs:
            early.wait()
        for pieces in made:
            for c in pieces:
                c.wait()

    return writer


def solution(mesh):
    size_x, size_y = mesh.shape["gx"], mesh.shape["gy"]

    def shards(e_field, h_field, psi, material, eps_table, sigma_table):
        _, rows_x, rows_y, depth_z = e_field.shape
        assert rows_x == 2 * PML and rows_y == 2 * PML and size_x > 1 and size_y > 1
        f32 = jnp.float32
        any_space = pl.BlockSpec(memory_space=pltpu.HBM)
        smem = pl.BlockSpec(memory_space=pltpu.SMEM)
        face_x = (2, rows_y, depth_z)
        face_y = (2, rows_x, depth_z)
        corner = (SUB, depth_z)
        faces = (face_x, face_y, face_x, face_y, corner, corner)
        padded = (3, rows_x + 1, rows_y + SUB, depth_z)
        cell = (rows_x, rows_y, depth_z)
        vmem = pl.BlockSpec(memory_space=pltpu.VMEM)
        strip = (2, 3, rows_x, SUB, depth_z)
        edge = (2, 3, rows_y, depth_z)
        held = (padded, padded, psi.shape, cell, cell, strip, edge)
        state = pl.pallas_call(
            make_kernel(size_x, size_y, rows_x, rows_y, depth_z),
            out_shape=[pltpu.VMEM(shape, f32) for shape in held],
            in_specs=[any_space] * 4 + [smem] * 2,
            out_specs=[vmem] * len(held),
            scratch_shapes=[
                pltpu.VMEM(cell, jnp.int32),
                pltpu.VMEM((2, 3, rows_x, depth_z), f32),
                pltpu.VMEM((3, rows_y + SUB, depth_z), f32),
                pltpu.VMEM((rows_x + SUB, depth_z), f32),
            ]
            + [pltpu.VMEM(f, f32) for f in faces]
            + [pltpu.VMEM((2,) + f, f32) for f in faces]
            + [
                pltpu.SemaphoreType.DMA((25,)),
                pltpu.SemaphoreType.DMA((8,)),
                pltpu.SemaphoreType.DMA((8, 2)),
            ],
            compiler_params=pltpu.CompilerParams(
                collective_id=0, has_side_effects=True, vmem_limit_bytes=48 << 20
            ),
        )(e_field, h_field, psi, material, eps_table, sigma_table)
        return pl.pallas_call(
            make_writer(size_x, size_y, rows_x, rows_y, depth_z),
            out_shape=[jax.ShapeDtypeStruct(a.shape, f32) for a in (e_field, h_field, psi)],
            in_specs=[vmem] * len(held),
            out_specs=[any_space] * 3,
            scratch_shapes=[
                pltpu.VMEM((3,) + cell, f32),
                pltpu.VMEM((6,) + cell, f32),
                pltpu.SemaphoreType.DMA((8 + 2 * (rows_x // GROUP),)),
            ],
            compiler_params=pltpu.CompilerParams(vmem_limit_bytes=32 << 20),
        )(*state)

    split = P(None, "gx", "gy", None)
    return jax.shard_map(
        shards,
        mesh=mesh,
        in_specs=(split, split, split, P("gx", "gy", None), P(), P()),
        out_specs=(split, split, split),
        check_vma=False,
    )
```

```python
import jax
import jax.numpy as jnp
from jax import lax
from jax.experimental import pallas as pl
from jax.experimental.pallas import tpu as pltpu
from jax.sharding import PartitionSpec as P

PML = 16
STEPS = 16
NMAT = 8
SUB = 8
GROUP = 16
AHEAD = 2

time_step = 0.5
sigma_peak = 3.0
kappa_peak = 5.0
alpha_peak = 0.05
MESH = pl.DeviceIdType.MESH


def profile(index, extent, shift_half):
    position = index.astype(jnp.float32) + shift_half
    slab_width = float(PML)
    depth_frac = jnp.maximum(
        jnp.maximum(
            (slab_width - position) / slab_width, (position - (extent - slab_width)) / slab_width
        ),
        0.0,
    )
    depth_cube = depth_frac * depth_frac * depth_frac
    sigma_value = sigma_peak * depth_cube
    kappa_value = 1.0 + (kappa_peak - 1.0) * depth_cube
    alpha_value = alpha_peak * (1.0 - depth_frac)
    decays = jnp.exp(-(sigma_value / kappa_value + alpha_value) * time_step)
    scaling = (
        sigma_value * (decays - 1.0) / (kappa_value * (sigma_value + kappa_value * alpha_value))
    )
    inside_slab = depth_frac > 0.0
    return (
        jnp.where(inside_slab, decays, 0.0),
        jnp.where(inside_slab, scaling, 0.0),
        1.0 / kappa_value,
    )


def make_cell(
    E, H, S, keep, drive, cx, cy, zc, slab_x, slab_y, tiles, depth_z, e_to, s_to, s_base
):
    lane = lax.broadcasted_iota(jnp.int32, (SUB, depth_z), 1)
    not_last = lane < depth_z - 1
    not_first = lane > 0

    def term(old, d, coef):
        b, a, q = coef
        renewed = b * old + a * d
        return q * d + renewed, renewed

    def loads(k, i, y, in_x, in_y):
        rows, at = pl.ds(y, SUB), pl.ds(y + SUB, SUB)
        first = 6 * k
        if k == 0:
            src, j, now, step, line = E, i, rows, 1, pl.ds(y + 1, SUB)
            old = [H[c, i + 1, at, :] for c in range(3)]
            mats = ()
        else:
            src, j, now, step, line = H, i + 1, at, -1, pl.ds(y + SUB - 1, SUB)
            old = [E[c, i, rows, :] for c in range(3)]
            mats = (keep[i, rows, :], drive[i, rows, :])
        own = [src[c, j, now, :] for c in range(3)]
        side_x = [src[c, j + step, now, :] for c in (1, 2)]
        side_y = [src[c, j, line, :] for c in (0, 2)]
        slots = [1, 2] + ([3, 4] if in_x else []) + ([0, 5] if in_y else [])
        aux = {n: S[first + n, i, rows, :] for n in slots}
        coef_x = [cx[k, n, i] for n in range(3)] if in_x else None
        return own, side_x, side_y, old, mats, aux, coef_x

    def compute(k, values, coef_y):
        own, (x1, x2), (y0, y2), old, mats, aux, coef_x = values
        f0, f1, f2 = own
        if k == 0:
            dx1, dx2, dy0, dy2 = x1 - f1, x2 - f2, y0 - f0, y2 - f2
            dz0 = jnp.where(not_last, pltpu.roll(f0, depth_z - 1, 1), 0.0) - f0
            dz1 = jnp.where(not_last, pltpu.roll(f1, depth_z - 1, 1), 0.0) - f1
        else:
            dx1, dx2, dy0, dy2 = f1 - x1, f2 - x2, f0 - y0, f2 - y2
            dz0 = f0 - jnp.where(not_first, pltpu.roll(f0, 1, 1), 0.0)
            dz1 = f1 - jnp.where(not_first, pltpu.roll(f1, 1, 1), 0.0)
        fresh = {}
        dz1, fresh[1] = term(aux[1], dz1, zc[k])
        dz0, fresh[2] = term(aux[2], dz0, zc[k])
        if coef_x is not None:
            dx2, fresh[3] = term(aux[3], dx2, coef_x)
            dx1, fresh[4] = term(aux[4], dx1, coef_x)
        if coef_y is not None:
            dy2, fresh[0] = term(aux[0], dy2, coef_y)
            dy0, fresh[5] = term(aux[5], dy0, coef_y)
        curls = (dy2 - dz1, dz0 - dx2, dx1 - dy0)
        if k == 0:
            return [o - time_step * c for o, c in zip(old, curls)], fresh
        return [mats[0] * o + mats[1] * c for o, c in zip(old, curls)], fresh

    def stores(k, i, y, result):
        fields, fresh = result
        for c in range(3):
            if k == 0:
                H[c, i + 1, pl.ds(y + SUB, SUB), :] = fields[c]
            else:
                e_to[c, i, pl.ds(y, SUB), :] = fields[c]
        for n, v in fresh.items():
            s_to[6 * k + n - s_base, i, pl.ds(y, SUB), :] = v

    def run(k, i0, y, in_x, in_y):
        coef_y = [cy[k, n, pl.ds(y, SUB), :] for n in range(3)] if in_y else None
        ready = [loads(k, i0 + u, y, in_x, in_y) for u in range(AHEAD)]
        for u in range(GROUP):
            if u + AHEAD < GROUP:
                ready.append(loads(k, i0 + u + AHEAD, y, in_x, in_y))
            stores(k, i0 + u, y, compute(k, ready[u], coef_y))

    def unit(k, g, t):
        low_x, low_y = g * GROUP < PML, t * SUB < PML
        px = jnp.where(low_x, slab_x[0], slab_x[1])
        py = jnp.where(low_y, slab_y[0], slab_y[1])
        i0, y = g * GROUP, pl.multiple_of(t * SUB, SUB)

        def split_y(in_x):
            lax.cond(
                py,
                lambda: run(k, i0, y, in_x, True),
                lambda: run(k, i0, y, in_x, False),
            )

        lax.cond(px, lambda: split_y(True), lambda: split_y(False))

    return loads, compute, unit


def make_kernel(size_x, size_y, rows_x, rows_y, depth_z):
    groups = rows_x // GROUP
    tiles = rows_y // SUB
    top, right = rows_x - 1, rows_y - 1

    def kernel(
        e_in, h_in, p_in, m_in, eps_ref, sig_ref, E, H, S,
        keep, drive, cx, cy, mat, cp, edge_x, edge_y, row_e, row_h, row_p,
        t_ex, t_ey, t_ax, t_ay, t_c0, t_c1,
        r_ex, r_ey, r_ax, r_ay, r_c0, r_c1,
        in_sem, send_sem, recv_sem,
    ):
        gx, gy = lax.axis_index("gx"), lax.axis_index("gy")
        has_lx, has_hx = gx > 0, gx < size_x - 1
        has_ly, has_hy = gy > 0, gy < size_y - 1
        slab_x = (gx == 0, gx == size_x - 1)
        slab_y = (gy == 0, gy == size_y - 1)
        lx, hx, ly, hy = gx - 1, gx + 1, gy - 1, gy + 1
        both = jnp.logical_and
        links = (
            (has_lx, (lx, gy)),
            (has_hx, (hx, gy)),
            (has_ly, (gx, ly)),
            (has_hy, (gx, hy)),
            (both(has_hx, has_ly), (hx, ly)),
            (both(has_lx, has_hy), (lx, hy)),
        )

        mid = pl.ds(0, rows_y)

        def e_copy(first, number, n):
            layers = pl.ds(first, number)
            return pltpu.make_async_copy(e_in.at[:, layers], E.at[:, layers, mid, :], in_sem.at[n])

        def h_copy(first, number, n):
            return pltpu.make_async_copy(
                h_in.at[:, pl.ds(first, number)],
                H.at[:, pl.ds(first + 1, number), pl.ds(SUB, rows_y), :],
                in_sem.at[n],
            )

        def slot_copies(k, first, number, n):
            layers, pair = pl.ds(first, number), pl.ds(6 * k + 1, 2)
            made = [
                (
                    None,
                    pltpu.make_async_copy(
                        p_in.at[pair, layers], S.at[pair, layers], in_sem.at[n]
                    ),
                )
            ]
            for side in (0, 1):
                rows = pl.ds(side * PML, PML)
                for j, slot in enumerate((6 * k, 6 * k + 5)):
                    made.append(
                        (
                            slab_y[side],
                            pltpu.make_async_copy(
                                p_in.at[slot, layers, rows],
                                S.at[slot, layers, rows],
                                in_sem.at[n + 1 + 2 * side + j],
                            ),
                        )
                    )
            return made

        def across_copies(k, n):
            pair = pl.ds(6 * k + 3, 2)
            made = []
            for side in (0, 1):
                layers = pl.ds(side * PML, PML)
                made.append(
                    (
                        slab_x[side],
                        pltpu.make_async_copy(
                            p_in.at[pair, layers], S.at[pair, layers], in_sem.at[n + side]
                        ),
                    )
                )
            return made

        def each(copies, act):
            for present, copy in copies:
                if present is None:
                    act(copy)
                else:

                    @pl.when(present)
                    def _():
                        act(copy)

        def begin(copies):
            each(copies, lambda copy: copy.start())

        def settle(copies):
            each(copies, lambda copy: copy.wait())

        rim = [(None, e_copy(top, 1, 0)), (None, h_copy(top, 1, 1))]
        rim += slot_copies(0, top, 1, 2) + [(None, e_copy(0, 1, 7))]
        rest = [(None, e_copy(1, top - 1, 8)), (None, h_copy(0, top, 9))]
        rest += slot_copies(0, 0, top, 10) + across_copies(0, 15)
        kinds = [(None, pltpu.make_async_copy(m_in, mat, in_sem.at[17]))]
        later = slot_copies(1, 0, rows_x, 18) + across_copies(1, 23)
        row_copies = [
            (e_in.at[0, :, 0], t_ey.at[0]),
            (e_in.at[2, :, 0], t_ey.at[1]),
            (e_in.at[:, :, right], row_e),
            (h_in.at[:, :, right], row_h),
            (p_in.at[pl.ds(1, 4), :, right], row_p),
        ]
        line = [
            (None, pltpu.make_async_copy(a, b, in_sem.at[25 + n]))
            for n, (a, b) in enumerate(row_copies)
        ]
        for copies in (rim, line, rest, kinds, later):
            begin(copies)

        barrier = pltpu.get_barrier_semaphore()
        for present, target in links:

            @pl.when(present)
            def _():
                pl.semaphore_signal(barrier, inc=1, device_id=target, device_id_type=MESH)

        zero = jnp.zeros((SUB, depth_z), jnp.float32)
        for side in (0, 1):

            @pl.when(jnp.logical_not(slab_y[side]))
            def _():
                @pl.loop(0, rows_x)
                def _(i):
                    for s in (0, 5, 6, 11):
                        S[s, i, pl.ds(side * PML, PML), :] = jnp.zeros(
                            (PML, depth_z), jnp.float32
                        )

        lane = lax.broadcasted_iota(jnp.int32, (SUB, depth_z), 1)
        row = lax.broadcasted_iota(jnp.int32, (rows_y, depth_z), 0)
        column = lax.broadcasted_iota(jnp.int32, (rows_x, depth_z), 0)
        zc = []
        for k, shift in enumerate((0.5, 0.0)):
            zc.append(profile(lane, depth_z, shift))
            for n, v in enumerate(profile(row + gy * rows_y, size_y * rows_y, shift)):
                cy[k, n] = v
            for n, v in enumerate(profile(column + gx * rows_x, size_x * rows_x, shift)):
                cp[k, n] = v

        def clear_rest():
            for side in (0, 1):

                @pl.when(jnp.logical_not(slab_x[side]))
                def _():
                    @pl.loop(side * PML, side * PML + PML)
                    def _(i):
                        for s in (3, 4, 9, 10):
                            S[s, i] = jnp.zeros((rows_y, depth_z), jnp.float32)

            for c in range(3):
                for t in range(tiles):
                    E[c, rows_x, pl.ds(t * SUB, SUB), :] = zero
                    H[c, 0, pl.ds(SUB + t * SUB, SUB), :] = zero

            @pl.loop(0, rows_x)
            def _(i):
                for c in range(3):
                    E[c, i, pl.ds(rows_y, SUB), :] = zero
                    H[c, i + 1, pl.ds(0, SUB), :] = zero

            plane = lax.broadcasted_iota(jnp.int32, (rows_x, SUB, depth_z), 0)
            for k, shift in enumerate((0.5, 0.0)):
                for n, v in enumerate(profile(plane + gx * rows_x, size_x * rows_x, shift)):
                    cx[k, n] = v

        def materials():
            keep_vals, drive_vals = [], []
            for m in range(NMAT):
                eps = jnp.full((SUB, depth_z), eps_ref[m], jnp.float32)
                sig = jnp.full((SUB, depth_z), sig_ref[m], jnp.float32)
                loss = sig * time_step / (2.0 * eps)
                keep_vals.append((1.0 - loss) / (1.0 + loss))
                drive_vals.append((time_step / eps) / (1.0 + loss))

            @pl.loop(0, rows_x)
            def _(i):
                for t in range(tiles):
                    rows = pl.ds(t * SUB, SUB)
                    number = mat[i, rows, :]
                    kv, dv = keep_vals[0], drive_vals[0]
                    for m in range(1, NMAT):
                        chosen = number == m
                        kv = jnp.where(chosen, keep_vals[m], kv)
                        dv = jnp.where(chosen, drive_vals[m], dv)
                    keep[i, rows, :] = kv
                    drive[i, rows, :] = dv

        loads, compute, unit = make_cell(
            E, H, S, keep, drive, cx, cy, zc, slab_x, slab_y, tiles, depth_z, E, S, 0
        )

        def exchange(s):
            one, last = pl.ds(0, 1), pl.ds(SUB - 1, 1)
            diag_c0, diag_c1 = both(has_hx, has_ly), both(has_lx, has_hy)
            moves = (
                (diag_c0, (hx, ly), diag_c1, t_c0.at[one], r_c0.at[s, one]),
                (has_hx, (hx, gy), has_lx, t_ax.at[1], r_ax.at[s, 1]),
                (has_hx, (hx, gy), has_lx, t_ax.at[0], r_ax.at[s, 0]),
                (diag_c1, (lx, hy), diag_c0, t_c1.at[last], r_c1.at[s, last]),
                (has_lx, (lx, gy), has_hx, t_ex.at[0], r_ex.at[s, 0]),
                (has_lx, (lx, gy), has_hx, t_ex.at[1], r_ex.at[s, 1]),
                (has_ly, (gx, ly), has_hy, t_ey, r_ey.at[s]),
                (has_hy, (gx, hy), has_ly, t_ay, r_ay.at[s]),
            )
            made = [
                (
                    sends,
                    gets,
                    pltpu.make_async_remote_copy(
                        src_ref=src,
                        dst_ref=dst,
                        send_sem=send_sem.at[n],
                        recv_sem=recv_sem.at[n, s],
                        device_id=target,
                        device_id_type=MESH,
                    ),
                )
                for n, (sends, target, gets, src, dst) in enumerate(moves)
            ]
            return made[:3], made[3:6], made[6:]

        own = pl.ds(0, rows_y)
        inner = pl.ds(SUB, rows_y)
        half = time_step
        wide = rows_y + SUB
        flat_e = E.reshape(3 * (rows_x + 1) * wide, depth_z)
        flat_h = H.reshape(3 * (rows_x + 1) * wide, depth_z)
        flat_s = S.reshape(12 * rows_x * rows_y, depth_z)
        flat_keep = keep.reshape(rows_x * rows_y, depth_z)
        flat_drive = drive.reshape(rows_x * rows_y, depth_z)
        packs = rows_x // SUB

        def across(c, i, y):
            return pl.ds((c * (rows_x + 1) + i) * wide + y, SUB, stride=wide)

        def within(c, i, y):
            return pl.ds((c * rows_x + i) * rows_y + y, SUB, stride=rows_y)

        def start(moves):
            for sends, _g, copy in moves:

                @pl.when(sends)
                def _():
                    copy.start()

        def arrived(moves):
            for _s, gets, copy in moves:

                @pl.when(gets)
                def _():
                    copy.wait_recv()

        def left(moves):
            for sends, _g, copy in moves:

                @pl.when(sends)
                def _():
                    copy.wait_send()

        def coefs_y(k, y):
            return [cy[k, n, pl.ds(y, SUB), :] for n in range(3)]

        def face_low(c):
            for t in range(tiles):
                y = t * SUB
                fields, _f = compute(1, loads(1, 0, y, False, True), coefs_y(1, y))
                t_ex[c - 1, pl.ds(y, SUB), :] = fields[c]
                if c == 1 and t == tiles - 1:
                    t_c1[...] = fields[1]

        def face_high():
            fields = []
            for t in range(tiles):
                y = t * SUB
                fields.append(compute(1, loads(1, top, y, False, True), coefs_y(1, y))[0])
            t_c0[...] = fields[0][0]
            for t in range(tiles):
                rows = pl.ds(t * SUB, SUB)
                edge_x[0, rows, :] = fields[t][0]
                edge_x[1, rows, :] = fields[t][1]
                edge_x[2, rows, :] = fields[t][2]

        def partial_high(c):
            for t in range(tiles):
                y = t * SUB
                rows, at = pl.ds(y, SUB), pl.ds(y + SUB, SUB)
                e_new = [edge_x[n, rows, :] for n in range(3)]
                old = [H[n, rows_x, at, :] for n in range(3)]
                aux = {n: S[n, top, rows, :] for n in (1, 2, 0, 5)}
                side_y = (edge_x[0, pl.ds(y + 1, SUB), :], zero)
                values = (e_new, (zero, zero), side_y, old, (), aux, None)
                fields, _f = compute(0, values, coefs_y(0, y))
                t_ax[c - 1, rows, :] = fields[c]

        def packed_e(r, u):
            i = u * SUB
            own_h = [flat_h[across(c, i + 1, SUB + r), :] for c in range(3)]
            side_x = [flat_h[across(c, i, SUB + r), :] for c in (1, 2)]
            side_y = [flat_h[across(c, i + 1, SUB + r - 1), :] for c in (0, 2)]
            old = [flat_e[across(c, i, r), :] for c in range(3)]
            mats = (flat_keep[within(0, i, r), :], flat_drive[within(0, i, r), :])
            aux = {n: flat_s[within(6 + n, i, r), :] for n in (1, 2, 3, 4)}
            coef_x = [cp[1, n, pl.ds(i, SUB), :] for n in range(3)]
            return compute(1, (own_h, side_x, side_y, old, mats, aux, coef_x), None)[0]

        def faces_y():
            late = []
            for u in range(packs):
                rows = pl.ds(u * SUB, SUB)
                fields = packed_e(0, u)
                t_ey[0, rows, :] = fields[0]
                t_ey[1, rows, :] = fields[2]
                late.append(packed_e(right, u))
            partial_y(late)

        def partial_y(e_new, first=False):
            for u in range(packs):
                edge_y[pl.ds(u * SUB, SUB), :] = e_new[u][1]
            for u in range(packs):
                i = u * SUB
                rows = pl.ds(i, SUB)
                if first:
                    old = [row_h[c, rows, :] for c in range(3)]
                    aux = {n: row_p[n - 1, rows, :] for n in (1, 2, 3, 4)}
                else:
                    old = [flat_h[across(c, i + 1, SUB + right), :] for c in range(3)]
                    aux = {n: flat_s[within(n, i, right), :] for n in (1, 2, 3, 4)}
                coef_x = [cp[0, n, rows, :] for n in range(3)]
                side_x = (edge_y[pl.ds(i + 1, SUB), :], zero)
                values = (e_new[u], side_x, (zero, zero), old, (), aux, coef_x)
                fields, _f = compute(0, values, None)
                t_ay[0, rows, :] = fields[0]
                t_ay[1, rows, :] = fields[2]

        def sweep(k, count):
            @pl.loop(0, count)
            def _(n):
                unit(k, lax.div(n, tiles), lax.rem(n, tiles))

        def fix_y(s):
            @pl.when(has_hy)
            def _():
                for u in range(packs):
                    i = u * SUB
                    rows = pl.ds(i, SUB)
                    a0, a2 = across(0, i + 1, SUB + right), across(2, i + 1, SUB + right)
                    flat_h[a0, :] = flat_h[a0, :] - half * r_ey[s, 1, rows, :]
                    flat_h[a2, :] = flat_h[a2, :] + half * r_ey[s, 0, rows, :]

            @pl.when(has_ly)
            def _():
                for u in range(packs):
                    i = u * SUB
                    rows = pl.ds(i, SUB)
                    e0, e2 = flat_e[across(0, i, 0), :], flat_e[across(2, i, 0), :]
                    flat_h[across(0, i + 1, SUB - 1), :] = r_ay[s, 0, rows, :] - half * e2
                    flat_h[across(2, i + 1, SUB - 1), :] = r_ay[s, 1, rows, :] + half * e0

        def fix_corner_high(s):
            edge = pl.ds(SUB - 1, 1)
            H[2, rows_x, edge, :] = H[2, rows_x, edge, :] - half * r_c1[s, pl.ds(SUB - 1, 1), :]

        def fix_high(s):
            H[1, rows_x, inner, :] = H[1, rows_x, inner, :] + half * r_ex[s, 1]
            H[2, rows_x, inner, :] = H[2, rows_x, inner, :] - half * r_ex[s, 0]

        def fix_low_2(s):
            H[2, 0, inner, :] = r_ax[s, 1] - half * E[1, 0, own, :]

        def fix_corner_low(s):
            edge = pl.ds(SUB + right, 1)
            H[2, 0, edge, :] = H[2, 0, edge, :] + half * r_c0[s, pl.ds(0, 1), :]

        def fix_low_1(s):
            H[1, 0, inner, :] = r_ax[s, 0] + half * E[2, 0, own, :]

        def when(present, act):
            @pl.when(present)
            def _():
                act()

        def arrive_high(s, came):
            corner, first, second = [copy for _s, _g, copy in came]

            @pl.when(has_ly)
            def _():
                corner.wait_recv()
                fix_corner_high(s)

            first.wait_recv()
            second.wait_recv()
            fix_high(s)

        def arrive_low_2(s, came):
            corner, first, _second = [copy for _s, _g, copy in came]
            first.wait_recv()
            fix_low_2(s)

            @pl.when(has_hy)
            def _():
                corner.wait_recv()
                fix_corner_low(s)

        def arrive_low_1(s, came):
            came[2][2].wait_recv()
            fix_low_1(s)

        odd = lax.rem(gx, 2) == 1

        def in_turn(high, low):
            when(both(odd, has_hx), high)
            when(has_lx, low)
            when(both(jnp.logical_not(odd), has_hx), high)

        count = groups * tiles
        edge_x[0, pl.ds(rows_y, SUB), :] = zero
        edge_y[pl.ds(rows_x, SUB), :] = zero
        settle(rim)
        t_c0[...] = E[0, top, pl.ds(0, SUB), :]
        for c in range(3):
            edge_x[c, own, :] = E[c, top, own, :]
        partial_high(2)
        partial_high(1)
        t_ex[0] = E[1, 0, own, :]
        t_ex[1] = E[2, 0, own, :]
        t_c1[...] = E[1, 0, pl.ds(rows_y - SUB, SUB), :]
        pl.semaphore_wait(barrier, sum(jnp.where(present, 1, 0) for present, _t in links))
        first_high, first_low, first_y = exchange(0)
        in_turn(lambda: start(first_high), lambda: start(first_low))
        settle(line)
        partial_y([[row_e[c, pl.ds(u * SUB, SUB), :] for c in range(3)] for u in range(packs)], True)
        start(first_y)
        clear_rest()
        settle(rest)
        sweep(0, count)
        settle(kinds)
        materials()
        settle(later)

        def advance(step, carry):
            s = lax.rem(step, 2)
            out_high, out_low, old_y = exchange(s)
            new_high, new_low, new_y = exchange(1 - s)
            arrived(old_y)
            fix_y(s)
            left(old_y)
            left(out_high)
            left(out_low)

            def high():
                corner, first, second = [copy for _s, _g, copy in new_high]
                arrive_high(s, out_low)
                face_high()
                partial_high(2)
                when(has_ly, corner.start)
                first.start()
                partial_high(1)
                second.start()

            def low():
                corner, first, second = [copy for _s, _g, copy in new_low]
                arrive_low_2(s, out_high)
                face_low(1)
                when(has_hy, corner.start)
                first.start()
                arrive_low_1(s, out_high)
                face_low(2)
                second.start()

            in_turn(high, low)
            faces_y()
            start(new_y)
            sweep(1, count)
            sweep(0, count)
            return carry

        lax.fori_loop(0, STEPS - 1, advance, 0)
        s = (STEPS - 1) % 2
        last_high, last_low, last_y = exchange(s)
        arrived(last_y)
        fix_y(s)

        def last_from_low():
            arrive_low_2(s, last_high)
            arrive_low_1(s, last_high)

        when(has_hx, lambda: arrive_high(s, last_low))
        when(has_lx, last_from_low)
        for moves in (last_y, last_low, last_high):
            left(moves)

    return kernel


def make_writer(size_x, size_y, rows_x, rows_y, depth_z):
    groups = rows_x // GROUP
    tiles = rows_y // SUB

    def writer(E, H, S, keep, drive, cx, cy, e_out, h_out, p_out, e_new, s_new, out_sem):
        gx, gy = lax.axis_index("gx"), lax.axis_index("gy")
        slab_x = (gx == 0, gx == size_x - 1)
        slab_y = (gy == 0, gy == size_y - 1)
        copy = pltpu.make_async_copy
        h_part = copy(H.at[:, pl.ds(1, rows_x), pl.ds(SUB, rows_y), :], h_out, out_sem.at[0])
        p_part = copy(S.at[pl.ds(0, 6)], p_out.at[pl.ds(0, 6)], out_sem.at[1])
        h_part.start()
        p_part.start()
        slabs = []
        for side in (0, 1):
            half, pair = pl.ds(side * PML, PML), pl.ds(9, 2)
            to, sem = p_out.at[pair, half], out_sem.at[2 + side]
            early = copy(S.at[pair, half], to, sem)
            slabs.append((slab_x[side], early, copy(s_new.at[pl.ds(3, 2), half], to, sem)))
            for j, slot in enumerate((6, 11)):
                to, sem = p_out.at[slot, :, half], out_sem.at[4 + 2 * side + j]
                early = copy(S.at[slot, :, half], to, sem)
                slabs.append((slab_y[side], early, copy(s_new.at[slot - 6, :, half], to, sem)))
        for inside, early, _late in slabs:

            @pl.when(jnp.logical_not(inside))
            def _():
                early.start()

        zc = [profile(lax.broadcasted_iota(jnp.int32, (SUB, depth_z), 1), depth_z, 0.0)] * 2
        _loads, _compute, unit = make_cell(
            E, H, S, keep, drive, cx, cy, zc, slab_x, slab_y, tiles, depth_z, e_new, s_new, 6
        )
        made = []
        for g in range(groups):
            layers, pair, one_two = pl.ds(g * GROUP, GROUP), pl.ds(7, 2), pl.ds(1, 2)
            made.append(
                [
                    copy(e_new.at[:, layers], e_out.at[:, layers], out_sem.at[8 + 2 * g]),
                    copy(s_new.at[one_two, layers], p_out.at[pair, layers], out_sem.at[9 + 2 * g]),
                ]
            )

            @pl.loop(0, tiles)
            def _(t):
                unit(1, g, t)

            if g > 0:
                for c in made[g - 1]:
                    c.start()
        h_part.wait()
        for c in made[-1]:
            c.start()
        for inside, _early, late in slabs:

            @pl.when(inside)
            def _():
                late.start()

        p_part.wait()
        for _inside, early, _late in slabs:
            early.wait()
        for pieces in made:
            for c in pieces:
                c.wait()

    return writer


def solution(mesh):
    size_x, size_y = mesh.shape["gx"], mesh.shape["gy"]

    def shards(e_field, h_field, psi, material, eps_table, sigma_table):
        _, rows_x, rows_y, depth_z = e_field.shape
        assert rows_x == 2 * PML and rows_y == 2 * PML and size_x > 1 and size_y > 1
        f32 = jnp.float32
        any_space = pl.BlockSpec(memory_space=pltpu.HBM)
        smem = pl.BlockSpec(memory_space=pltpu.SMEM)
        face_x = (2, rows_y, depth_z)
        face_y = (2, rows_x, depth_z)
        corner = (SUB, depth_z)
        faces = (face_x, face_y, face_x, face_y, corner, corner)
        padded = (3, rows_x + 1, rows_y + SUB, depth_z)
        cell = (rows_x, rows_y, depth_z)
        vmem = pl.BlockSpec(memory_space=pltpu.VMEM)
        strip = (2, 3, rows_x, SUB, depth_z)
        edge = (2, 3, rows_y, depth_z)
        held = (padded, padded, psi.shape, cell, cell, strip, edge)
        state = pl.pallas_call(
            make_kernel(size_x, size_y, rows_x, rows_y, depth_z),
            out_shape=[pltpu.VMEM(shape, f32) for shape in held],
            in_specs=[any_space] * 4 + [smem] * 2,
            out_specs=[vmem] * len(held),
            scratch_shapes=[
                pltpu.VMEM(cell, jnp.int32),
                pltpu.VMEM((2, 3, rows_x, depth_z), f32),
                pltpu.VMEM((3, rows_y + SUB, depth_z), f32),
                pltpu.VMEM((rows_x + SUB, depth_z), f32),
                pltpu.VMEM((3, rows_x, depth_z), f32),
                pltpu.VMEM((3, rows_x, depth_z), f32),
                pltpu.VMEM((4, rows_x, depth_z), f32),
            ]
            + [pltpu.VMEM(f, f32) for f in faces]
            + [pltpu.VMEM((2,) + f, f32) for f in faces]
            + [
                pltpu.SemaphoreType.DMA((30,)),
                pltpu.SemaphoreType.DMA((8,)),
                pltpu.SemaphoreType.DMA((8, 2)),
            ],
            compiler_params=pltpu.CompilerParams(
                collective_id=0, has_side_effects=True, vmem_limit_bytes=48 << 20
            ),
        )(e_field, h_field, psi, material, eps_table, sigma_table)
        return pl.pallas_call(
            make_writer(size_x, size_y, rows_x, rows_y, depth_z),
            out_shape=[jax.ShapeDtypeStruct(a.shape, f32) for a in (e_field, h_field, psi)],
            in_specs=[vmem] * len(held),
            out_specs=[any_space] * 3,
            scratch_shapes=[
                pltpu.VMEM((3,) + cell, f32),
                pltpu.VMEM((6,) + cell, f32),
                pltpu.SemaphoreType.DMA((8 + 2 * (rows_x // GROUP),)),
            ],
            compiler_params=pltpu.CompilerParams(vmem_limit_bytes=32 << 20),
        )(*state)

    split = P(None, "gx", "gy", None)
    return jax.shard_map(
        shards,
        mesh=mesh,
        in_specs=(split, split, split, P("gx", "gy", None), P(), P()),
        out_specs=(split, split, split),
        check_vma=False,
    )
```
